256 devices in a mesh: band: 32 (over z, y_hi, core), chan: 8 (over x, y_lo).
Axes of the slice: x: 4, y: 4 (y_hi: 2, y_lo: 2; y = y_hi * 2 + y_lo), z: 8, core: 2. Of those that a mesh axis runs over, the one named last changes fastest.
Arguments:
- fine_features: bfloat16 [2, 192, 256, 512], P(None, 'chan', 'band'), may hold values from -100 to 100
- coarse_level: bfloat16 [2, 256, 128, 256], P(None, 'chan', 'band'), may hold values from -100 to 100
- lat_weight: bfloat16 [256, 192], P('chan'), may hold values from -0.4375 to 0.4375
- lat_gain: bfloat16 [256], P('chan'), may hold values from 0.099609375 to 1.8984375
- lat_shift: bfloat16 [256], P('chan'), may hold values from -3 to 3
- out_weight: bfloat16 [3, 3, 256, 256], P(None, None, 'chan'), may hold values from -0.125 to 0.125
- out_gain: bfloat16 [256], P('chan'), may hold values from 0.099609375 to 1.8984375
- out_shift: bfloat16 [256], P('chan'), may hold values from -3 to 3
- mask_weight: bfloat16 [256, 256], P('chan'), may hold values from -0.375 to 0.375
- mask_bias: bfloat16 [256], P('chan'), may hold values from -1.796875 to 1.796875
- queries: bfloat16 [200, 256], replicated, may hold values from -128 to 128
Outputs:
- log_probs: float32 [2, 200, 256, 512], P(None, None, ('band', 'chan'))
The draws below stay inside these ranges and needn't reach their ends.
All inputs are finite; a program needn't handle non-finite values.
Results may differ from the reference program's by a relative error of at most 0.0058.
Values may be sent and summed in bfloat16 or wider, within the bound.
A program may use at most 64 MiB of HBM per device.

```python
import jax
import jax.numpy as jnp
from jax import lax

D = 256
C4 = 192
QUERIES = 200
GROUPS = 32
IMAGES = 2
COLS = 512
H4 = 256


def banded_field(key, images, channels, height, width):
    key_noise = jax.random.fold_in(key, 0)
    key_rows = jax.random.fold_in(key, 1)
    key_cols = jax.random.fold_in(key, 2)
    key_offset = jax.random.fold_in(key, 4)
    positions = jnp.arange(height, dtype=jnp.float32) / max(height - 1, 1)
    ramp = 3.0 ** positions
    row_scale = ramp[None, :] * jnp.exp(jax.random.uniform(key_rows, (images, height), jnp.float32, -0.8, 0.8))
    col_scale = jnp.exp(jax.random.uniform(key_cols, (images, width), jnp.float32, -0.8, 0.8))
    scale = row_scale[:, None, :, None] * col_scale[:, None, None, :]
    offset = jax.random.uniform(key_offset, (images, channels, 1, 1), jnp.float32, -3.0, 3.0)
    noise = jax.random.truncated_normal(key_noise, -4.0, 4.0, (images, channels, height, width), jnp.float32)
    values = noise * scale + offset * ramp[None, None, :, None]
    return values


def draw_fine_features(key, part):
    return banded_field(jax.random.fold_in(key, 11), IMAGES, C4, H4, COLS).astype(jnp.bfloat16)


def draw_coarse_level(key, part):
    return banded_field(jax.random.fold_in(key, 12), IMAGES, D, H4 // 2, COLS // 2).astype(jnp.bfloat16)


def draw_queries(key, part):
    key_base = jax.random.fold_in(jax.random.fold_in(key, 13), 0)
    values = 0.25 * jax.random.truncated_normal(key_base, -4.0, 4.0, (QUERIES, D), jnp.float32)
    return values.astype(jnp.bfloat16)


def levels(own_key, extent, shards, smallest, high):
    factor_of = 1.0
    for axis_at, parts in shards:
        heights = jax.random.uniform(jax.random.fold_in(jax.random.fold_in(own_key, 6), axis_at), (parts,), jnp.float32, smallest / len(shards), high / len(shards))
        factor_of = factor_of * jnp.repeat(jnp.exp(heights), extent[axis_at] // parts).reshape((-1,) + (1,) * (len(extent) - 1 - axis_at))
    return factor_of


def bell_draw(stream_key, shape, spread, most, pieces=(), kind=jnp.bfloat16):
    values = jax.random.normal(stream_key, shape, jnp.float32) * spread
    if len(pieces) > 0:
        values = levels(stream_key, shape, pieces, -0.22, 0.18) * values
    return jnp.clip(values, min=-most, max=most).astype(kind)


def setup_inputs(seed: int = 0) -> dict:
    key_of = jax.random.split(jax.random.key(seed), 12)
    return {
        "fine_features": draw_fine_features(jax.random.fold_in(key_of[11], 71), 0),
        "coarse_level": draw_coarse_level(jax.random.fold_in(key_of[11], 71), 0),
        "lat_weight": bell_draw(key_of[2], (D, C4), C4 ** -0.5, 0.4375, ((0, 8),)),
        "lat_gain": jnp.clip(1.0 + 0.18 * jax.random.normal(key_of[3], (D,), jnp.float32), 0.099609375, 1.8984375).astype(jnp.bfloat16),
        "lat_shift": bell_draw(key_of[4], (D,), 0.5, 3.0, ((0, 8),)),
        "out_weight": bell_draw(key_of[5], (3, 3, D, D), (9 * D) ** -0.5, 0.125, ((2, 8),)),
        "out_gain": jnp.clip(1.0 + 0.18 * jax.random.normal(key_of[6], (D,), jnp.float32), 0.099609375, 1.8984375).astype(jnp.bfloat16),
        "out_shift": bell_draw(key_of[7], (D,), 0.5, 3.0, ((0, 8),)),
        "mask_weight": bell_draw(key_of[8], (D, D), D ** -0.5, 0.375, ((0, 8),)),
        "mask_bias": bell_draw(key_of[9], (D,), 0.3, 1.796875, ((0, 8),)),
        "queries": draw_queries(jax.random.fold_in(key_of[11], 71), 0),
    }


epsilon = 1e-05

def interp(padded, axis):
    length = padded.shape[axis] - 2
    before = lax.slice_in_dim(padded, 0, length, axis=axis)
    middle = lax.slice_in_dim(padded, 1, length + 1, axis=axis)
    after = lax.slice_in_dim(padded, 2, length + 2, axis=axis)
    even_part = 0.25 * before + 0.75 * middle
    odd_part = 0.75 * middle + 0.25 * after
    paired = jnp.stack([even_part, odd_part], axis + 1)
    new_shape = list(middle.shape)
    new_shape[axis] = 2 * length
    return paired.reshape(new_shape)

def group_norm(values, gain, shift, group_size):
    channels, height, width = values.shape
    blocks = values.reshape(channels // group_size, group_size * height * width)
    mean_value = lax.optimization_barrier(jnp.mean(blocks, axis=1, keepdims=True))
    deviation = blocks - mean_value
    variance = lax.optimization_barrier(jnp.mean(deviation * deviation, axis=1, keepdims=True))
    scaled = ((blocks - mean_value) * lax.rsqrt(variance + epsilon)).reshape(channels, height, width)
    return scaled * gain.astype(jnp.float32)[:, None, None] + shift.astype(jnp.float32)[:, None, None]

def reference(fine_features, coarse_level, lat_weight, lat_gain, lat_shift, out_weight, out_gain, out_shift, mask_weight, mask_bias, queries):
    group_size = D // GROUPS

    def one_image(pair):
        fine_image, coarse_image = pair
        lateral = jnp.dot(lat_weight, fine_image.reshape(C4, H4 * COLS), preferred_element_type=jnp.float32).reshape(D, H4, COLS)
        lat_normed = group_norm(lateral, lat_gain, lat_shift, group_size)
        extended = jnp.pad(coarse_image.astype(jnp.float32), ((0, 0), (1, 1), (1, 1)), mode='edge')
        upsampled = interp(interp(extended, 1), 2)
        joined = (lat_normed + upsampled).astype(jnp.bfloat16)
        padded = jnp.pad(joined, ((0, 0), (1, 1), (1, 1)))
        conv_out = jnp.zeros((D, H4 * COLS), jnp.float32)
        for row_tap in range(3):
            for col_tap in range(3):
                window = padded[:, row_tap:row_tap + H4, col_tap:col_tap + COLS].reshape(D, H4 * COLS)
                conv_out = conv_out + jnp.dot(out_weight[row_tap, col_tap], window, preferred_element_type=jnp.float32)
        conv_out = conv_out.reshape(D, H4, COLS)
        activated = jnp.maximum(group_norm(conv_out, out_gain, out_shift, group_size), 0.0).astype(jnp.bfloat16)
        features = jnp.dot(mask_weight, activated.reshape(D, H4 * COLS), preferred_element_type=jnp.float32)
        features = (features + mask_bias.astype(jnp.float32)[:, None]).astype(jnp.bfloat16)
        logits = jnp.dot(queries, features, preferred_element_type=jnp.float32)
        peak = lax.optimization_barrier(jnp.max(logits, axis=0, keepdims=True))
        shifted = logits - peak
        result = shifted - jnp.log(lax.optimization_barrier(jnp.sum(jnp.exp(shifted), axis=0, keepdims=True)))
        return result.reshape(QUERIES, H4, COLS)
    return lax.map(one_image, (fine_features, coarse_level))
```

```python
import functools

import jax
import jax.numpy as jnp
from jax import lax
from jax.experimental import pallas as pl
from jax.experimental.pallas import tpu as pltpu
from jax.sharding import Mesh
from jax.sharding import PartitionSpec as P

D = 256
GROUPS = 32
COLS = 512
AXES = ("band_0", "band_1", "band_2", "chan_0", "chan_1")
BAND = AXES[:3]
CHAN = AXES[3:]
MESH = pl.DeviceIdType.MESH
f32, bf16 = jnp.float32, jnp.bfloat16
epsilon = 1e-05

CHAN_OFF = [(dx, dy) for dx in (1, 3, 2, 0) for dy in (0, 1) if (dx, dy) != (0, 0)]
PLANE_OFF = [
    (dx, dh, dl)
    for dx in (2, 1, 3, 0)
    for dh in (1, 0)
    for dl in (1, 0)
    if (dx, dh, dl) != (0, 0, 0)
]
LINE_OFF = [(dz, dc) for dz in (4, 3, 5, 2, 6, 1, 7, 0) for dc in (1, 0) if (dz, dc) != (0, 0)]


def kernel(
    pixels,
    fine, coarse, latw, lat_gain, lat_shift, outw, out_gain, out_shift, maskw, mask_bias, queries,
    out,
    X, C, WL, WC, PB, pstage, LAT, UPS, JS, CO, RC,
    plane_src, plane_dst, line_src, line_dst,
    s_fine, r_fine, s_coarse, r_coarse, s_latw, r_latw, s_par, r_par, s_w, r_w, s_m, r_m,
    s_halo, r_halo, s_core, r_core, s_plane, r_plane, s_line, r_line, s_row, r_row,
):
    z, yh, core = (lax.axis_index(a) for a in BAND)
    x, yl = (lax.axis_index(a) for a in CHAN)
    me = x * 2 + yl
    pair = ((z * 2 + yh) * 2 + core) * 4 + x

    def chan_peer(dx, dy):
        return (z, yh, core, lax.rem(x + dx, 4), lax.rem(yl + dy, 2))

    def plane_peer(dx, dh, dl):
        return (z, lax.rem(yh + dh, 2), core, lax.rem(x + dx, 4), lax.rem(yl + dl, 2))

    def line_peer(dz, dc):
        return (lax.rem(z + dz, 8), yh, lax.rem(core + dc, 2), x, yl)

    def pair_owner(g):
        b = lax.div(g, 4)
        return (lax.div(b, 4), lax.rem(lax.div(b, 2), 2), lax.rem(b, 2), lax.rem(g, 4), yl)

    above = pair_owner(lax.rem(pair + 127, 128))
    below = pair_owner(lax.rem(pair + 1, 128))
    partner = (z, yh, 1 - core, x, yl)
    other = (z, yh, core, x, 1 - yl)

    def remote(src, dst, send, recv, dev):
        return pltpu.make_async_remote_copy(
            src_ref=src, dst_ref=dst, send_sem=send, recv_sem=recv,
            device_id=dev, device_id_type=MESH,
        )

    barrier = pltpu.get_barrier_semaphore()
    for dev in [plane_peer(*o) for o in PLANE_OFF] + [line_peer(*o) for o in LINE_OFF] + [above, below]:
        pl.semaphore_signal(barrier, inc=1, device_id=dev, device_id_type=MESH)
    pstage[...] = jnp.zeros_like(pstage)
    for j, ref in enumerate((lat_gain, lat_shift, out_gain, out_shift, mask_bias)):
        pstage[j : j + 1, 0:32] = ref[...].astype(f32)
    PB[me] = pstage[...]
    WL[me] = latw[...]
    X[pl.ds(1, 2), me] = fine[yl, pl.ds(2 * x, 2)]
    C[1, me] = coarse[yl, x]
    WC[pl.ds(0, 9), me, core] = outw[:, core]
    WC[9, me, core] = maskw[core]
    pl.semaphore_wait(barrier, len(PLANE_OFF) + len(LINE_OFF) + 2)

    fine_c, coarse_c, latw_c, par_c, w_c, m_c = [], [], [], [], [], []
    for k, o in enumerate(CHAN_OFF):
        dev = chan_peer(*o)
        fine_c.append(remote(fine.at[dev[4], pl.ds(2 * dev[3], 2)], X.at[pl.ds(1, 2), me],
                             s_fine.at[k], r_fine.at[k], dev))
        latw_c.append(remote(latw, WL.at[me], s_latw.at[k], r_latw.at[k], dev))
        par_c.append(remote(pstage, PB.at[me], s_par.at[k], r_par.at[k], dev))
        coarse_c.append(remote(coarse.at[dev[4], dev[3]], C.at[1, me],
                               s_coarse.at[k], r_coarse.at[k], dev))
        w_c.append(remote(outw.at[:, core], WC.at[pl.ds(0, 9), me, core], s_w.at[k], r_w.at[k], dev))
        m_c.append(remote(maskw.at[core], WC.at[9, me, core], s_m.at[k], r_m.at[k], dev))
    for group in (latw_c, fine_c, par_c, coarse_c):
        for c in group:
            c.start()

    ci = lax.broadcasted_iota(jnp.int32, (256, COLS), 0)
    cj = lax.broadcasted_iota(jnp.int32, (256, COLS), 1)
    center = lax.shift_right_logical(cj, 1)
    side = jnp.clip(jnp.where(lax.bitwise_and(cj, 1) == 0, center - 1, center + 1), 0, 255)
    widen = (jnp.where(ci == center, 0.75, 0.0) + jnp.where(ci == side, 0.25, 0.0)).astype(bf16)

    def lateral_of(slot):
        rows = X[slot].astype(f32).reshape(192, COLS).astype(bf16)
        return jnp.dot(WL[...].astype(f32).reshape(256, 192).astype(bf16), rows,
                       preferred_element_type=f32)

    def row_stats(rows):
        s = q = None
        for row in rows:
            for k in range(COLS // 128):
                t = row[:, 128 * k : 128 * (k + 1)]
                s = t if s is None else s + t
                q = t * t if q is None else q + t * t
        both = jnp.concatenate(
            [jnp.sum(s.reshape(GROUPS, 8, 128), 1), jnp.sum(q.reshape(GROUPS, 8, 128), 1),
             jnp.zeros((64, 128), f32)], 0)
        return jnp.sum(jnp.transpose(both), 0, keepdims=True)

    def scale_shift(total, gain, shift):
        tall = jnp.transpose(jnp.broadcast_to(total, (128, 128)))
        mean = tall[0:32] / pixels
        var = tall[32:64] / pixels - mean * mean
        rstd = lax.rsqrt(var + epsilon)
        spread = lambda v: jnp.broadcast_to(v[:, None, :], (GROUPS, 8, 128)).reshape(D, 128)
        a = spread(rstd) * gain
        return a, shift - spread(mean) * a

    def send_plane(it, stats, offsets):
        plane_src[it] = stats
        done = []
        for k, o in enumerate(PLANE_OFF):
            if o in offsets:
                c = remote(plane_src.at[it], plane_dst.at[it, k], s_plane.at[it, k],
                           r_plane.at[it, k], plane_peer(*o))
                c.start()
                done.append(c)
        return done

    def send_line(it):
        done = []
        for k, o in enumerate(LINE_OFF):
            c = remote(line_src.at[it], line_dst.at[it, k], s_line.at[it, k],
                       r_line.at[it, k], line_peer(*o))
            c.start()
            done.append(c)
        return done

    def line_total(it):
        t = line_src[it]
        for k in range(len(LINE_OFF)):
            t = t + line_dst[it, k]
        return t

    for c in latw_c:
        c.wait_recv()
    for c in fine_c:
        c.wait_recv()
    own_rows = [lateral_of(1), lateral_of(2)]
    LAT[1] = own_rows[0]
    LAT[2] = own_rows[1]
    same = [o for o in PLANE_OFF if o[2] == 0]
    first_stats = row_stats(own_rows)
    plane1 = send_plane(0, first_stats, same)

    halo_c = [
        remote(X.at[1], X.at[3], s_halo.at[0], r_halo.at[0], above),
        remote(X.at[2], X.at[0], s_halo.at[1], r_halo.at[1], below),
    ]
    for c in halo_c:
        c.start()
    for c in w_c + m_c:
        c.start()
    for c in coarse_c:
        c.wait_recv()
    coarse_halo = [
        remote(C.at[1], C.at[2], s_halo.at[2], r_halo.at[2], above),
        remote(C.at[1], C.at[0], s_halo.at[3], r_halo.at[3], below),
    ]
    for c in coarse_halo:
        c.start()

    for c in plane1:
        c.wait_recv()
    t = first_stats
    for k, o in enumerate(PLANE_OFF):
        if o in same:
            t = t + plane_dst[0, k]
    line_src[0] = jnp.concatenate([t, jnp.zeros((1, 128), f32)], 0)
    line1 = send_line(0)

    for c in par_c:
        c.wait_recv()
    turned = jnp.transpose(jnp.concatenate([PB[...].reshape(64, 128), jnp.zeros((64, 128), f32)], 0))

    def param(j):
        col = jnp.concatenate([turned[0:32, 8 * s + j : 8 * s + j + 1] for s in range(8)], 0)
        return jnp.broadcast_to(col, (D, 128))

    for c in halo_c:
        c.wait_recv()
    LAT[0] = lateral_of(0)
    LAT[3] = lateral_of(3)
    for c in coarse_halo:
        c.wait_recv()
    wide = [jnp.dot(C[s].reshape(256, 256), widen, preferred_element_type=f32) for s in range(3)]
    top = jnp.where(pair == 0, wide[1], wide[0])
    bottom = jnp.where(pair == 127, wide[1], wide[2])
    UPS[0] = 0.75 * top + 0.25 * wide[1]
    UPS[1] = 0.25 * top + 0.75 * wide[1]
    UPS[2] = 0.75 * wide[1] + 0.25 * bottom
    UPS[3] = 0.25 * wide[1] + 0.75 * bottom

    for c in w_c + m_c:
        c.wait_recv()
    core_c = remote(WC.at[:, :, core], WC.at[:, :, core], s_core, r_core, partner)
    core_c.start()

    for c in line1:
        c.wait_recv()
    a, b = scale_shift(line_total(0)[0:1], param(0), param(1))
    a4 = jnp.concatenate([a] * 4, 1)
    b4 = jnp.concatenate([b] * 4, 1)
    lane = lax.broadcasted_iota(jnp.int32, (D, COLS), 1)
    for s in range(4):
        j = LAT[s] * a4 + b4 + UPS[s]
        if s == 0:
            j = jnp.where(pair == 0, 0.0, j)
        if s == 3:
            j = jnp.where(pair == 127, 0.0, j)
        cols = slice(COLS * s, COLS * (s + 1))
        JS[0:256, cols] = jnp.where(lane == 0, 0.0, pltpu.roll(j, 1, 1)).astype(bf16)
        JS[256:512, cols] = j.astype(bf16)
        JS[512:768, cols] = jnp.where(lane == COLS - 1, 0.0, pltpu.roll(j, COLS - 1, 1)).astype(bf16)

    core_c.wait_recv()
    acc = None
    for tap in range(3):
        w = jnp.concatenate([WC[3 * tap + i].reshape(256, 256) for i in range(3)], 1)
        term = jnp.dot(w, JS[:, COLS * tap : COLS * (tap + 2)], preferred_element_type=f32)
        acc = term if acc is None else acc + term
    CO[0] = acc[:, :COLS].astype(bf16)
    CO[1] = acc[:, COLS:].astype(bf16)
    second_stats = row_stats([acc[:, :COLS], acc[:, COLS:]])
    plane2 = send_plane(1, second_stats, PLANE_OFF)
    row_c = remote(CO.at[1 - yl], RC, s_row, r_row, other)
    row_c.start()
    for c in plane2:
        c.wait_recv()
    mine, others = second_stats, None
    for k, o in enumerate(PLANE_OFF):
        v = plane_dst[1, k]
        if o[2] == 0:
            mine = mine + v
        else:
            others = v if others is None else others + v
    line_src[1] = jnp.concatenate([mine, others], 0)
    line2 = send_line(1)
    for c in line2:
        c.wait_recv()
    total = line_total(1)
    gain2, shift2, bias = param(2), param(3), param(4)
    bias4 = jnp.concatenate([bias] * 4, 1)
    mask_w = WC[9].reshape(256, 256)
    row_c.wait_recv()
    for who in range(2):
        a, b = scale_shift(total[who : who + 1], gain2, shift2)
        row = CO[yl] if who == 0 else RC[...]
        act = jnp.maximum(
            row.astype(f32) * jnp.concatenate([a] * 4, 1) + jnp.concatenate([b] * 4, 1), 0.0
        ).astype(bf16)
        feat = (jnp.dot(mask_w, act, preferred_element_type=f32) + bias4).astype(bf16)
        logits = jnp.dot(queries[...], feat, preferred_element_type=f32)
        shifted = logits - jnp.max(logits, 0, keepdims=True)
        res = shifted - jnp.log(jnp.sum(jnp.exp(shifted), 0, keepdims=True))
        out[yl if who == 0 else 1 - yl] = res

    for group in (fine_c, latw_c, par_c, coarse_c, w_c, m_c, halo_c, coarse_halo, plane1, plane2,
                  line1, line2, [core_c, row_c]):
        for c in group:
            c.wait_send()


def per_device(
    fine_features, coarse_level, lat_weight, lat_gain, lat_shift, out_weight, out_gain, out_shift,
    mask_weight, mask_bias, queries,
):
    pixels = float(D // GROUPS * 256 * COLS)
    fine = jnp.transpose(fine_features, (0, 2, 1, 3))
    coarse = jnp.transpose(coarse_level, (0, 2, 1, 3))
    vec = lambda v: v.reshape(1, 32)
    V = pltpu.VMEM
    dma = pltpu.SemaphoreType.DMA
    out = pl.pallas_call(
        functools.partial(kernel, pixels),
        out_shape=jax.ShapeDtypeStruct((2, 200, COLS), f32),
        in_specs=[pl.BlockSpec(memory_space=V)] * 11,
        out_specs=pl.BlockSpec(memory_space=V),
        scratch_shapes=[
            V((4, 8, 24, COLS), bf16),
            V((3, 8, 32, 256), bf16),
            V((8, 32, 192), bf16),
            V((10, 8, 2, 16, 256), bf16),
            V((8, 8, 128), f32),
            V((8, 128), f32),
            V((4, D, COLS), f32),
            V((4, D, COLS), f32),
            V((3 * D, 4 * COLS), bf16),
            V((2, D, COLS), bf16),
            V((D, COLS), bf16),
            V((2, 1, 128), f32),
            V((2, 15, 1, 128), f32),
            V((2, 2, 128), f32),
            V((2, 15, 2, 128), f32),
        ]
        + [dma((7,))] * 12
        + [dma((4,))] * 2
        + [dma] * 2
        + [dma((2, 15))] * 4
        + [dma] * 2,
        compiler_params=pltpu.CompilerParams(
            collective_id=0, has_side_effects=True, vmem_limit_bytes=56 * 1024 * 1024
        ),
        name="merge",
    )(
        fine, coarse, lat_weight, vec(lat_gain), vec(lat_shift),
        out_weight.reshape(9, 2, 16, 256), vec(out_gain), vec(out_shift),
        mask_weight.reshape(2, 16, 256), vec(mask_bias), queries,
    )
    return out.reshape(2, 200, 1, COLS)


def solution(mesh):
    finer = Mesh(mesh.devices.reshape(8, 2, 2, 4, 2), AXES)
    return jax.shard_map(
        per_device,
        mesh=finer,
        in_specs=(
            P(None, CHAN, BAND, None),
            P(None, CHAN, BAND, None),
            P(CHAN, None),
            P(CHAN),
            P(CHAN),
            P(None, None, CHAN, None),
            P(CHAN),
            P(CHAN),
            P(CHAN, None),
            P(CHAN),
            P(),
        ),
        out_specs=P(None, None, AXES, None),
        check_vma=False,
    )
```

```python
import functools

import jax
import jax.numpy as jnp
from jax import lax
from jax.experimental import pallas as pl
from jax.experimental.pallas import tpu as pltpu
from jax.sharding import Mesh
from jax.sharding import PartitionSpec as P

D = 256
GROUPS = 32
COLS = 512
AXES = ("band_0", "band_1", "band_2", "chan_0", "chan_1")
BAND = AXES[:3]
CHAN = AXES[3:]
MESH = pl.DeviceIdType.MESH
f32, bf16 = jnp.float32, jnp.bfloat16
epsilon = 1e-05

CHAN_OFF = [(dx, dy) for dx in (2, 1, 3, 0) for dy in (1, 0) if (dx, dy) != (0, 0)]
PLANE_OFF = [
    (dx, dh, dl)
    for dx in (2, 1, 3, 0)
    for dh in (1, 0)
    for dl in (1, 0)
    if (dx, dh, dl) != (0, 0, 0)
]
SAME_OFF = [o for o in PLANE_OFF if o[2] == 0]
LINE_OFF = [(dz, dc) for dz in (4, 3, 5, 2, 6, 1, 7, 0) for dc in (1, 0) if (dz, dc) != (0, 0)]
DEST = [(xh, dc, dl) for xh in (0, 1) for dc in (0, 1) for dl in (0, 1)]


def kernel(
    pixels,
    fine, coarse, latw, lat_gain, lat_shift, outw, out_gain, out_shift, maskw, mask_bias, queries,
    out,
    FS, FB, CB, WB, X, C, WL, WC, PB, pstage, LAT, UPS, JS, CO, R,
    plane_src, plane_dst, line_src, line_dst,
    s_fine, r_fine, s_coarse, r_coarse, s_latw, r_latw, s_par, r_par, s_w, r_w,
    s_halo, r_halo, s_z, r_z, s_core, r_core, s_plane, r_plane, s_line, r_line, s_row, r_row,
):
    z, yh, core = (lax.axis_index(a) for a in BAND)
    x, yl = (lax.axis_index(a) for a in CHAN)
    me = x * 2 + yl
    pair = (z * 2 + yh) * 8 + x * 2 + core
    half = lax.rem(z, 2)

    def chan_peer(dx, dy, dc=0):
        return (z, yh, lax.rem(core + dc, 2), lax.rem(x + dx, 4), lax.rem(yl + dy, 2))

    def plane_peer(dx, dh, dl):
        return (z, lax.rem(yh + dh, 2), core, lax.rem(x + dx, 4), lax.rem(yl + dl, 2))

    def line_peer(dz, dc):
        return (lax.rem(z + dz, 8), yh, lax.rem(core + dc, 2), x, yl)

    def pair_owner(g):
        k, p = lax.div(g, 8), lax.rem(g, 8)
        return (lax.div(k, 2), lax.rem(k, 2), lax.rem(p, 2), lax.div(p, 2), yl)

    above = pair_owner(lax.rem(pair + 127, 128))
    below = pair_owner(lax.rem(pair + 1, 128))
    partner = (z, yh, 1 - core, x, yl)

    def remote(src, dst, send, recv, dev):
        return pltpu.make_async_remote_copy(
            src_ref=src, dst_ref=dst, send_sem=send, recv_sem=recv,
            device_id=dev, device_id_type=MESH,
        )

    barrier = pltpu.get_barrier_semaphore()
    peers = (
        [plane_peer(*o) for o in PLANE_OFF]
        + [line_peer(*o) for o in LINE_OFF]
        + [chan_peer(*o, 1) for o in CHAN_OFF]
        + [above, below]
    )
    for dev in peers:
        pl.semaphore_signal(barrier, inc=1, device_id=dev, device_id_type=MESH)

    for k in range(4):
        cols = slice(128 * k, 128 * (k + 1))
        FS[384 * k : 384 * (k + 1)] = fine[:, cols].astype(f32)
        for n in range(2):
            for r in range(8):
                FB[n, r, :, cols] = FS[pl.ds(384 * k + 192 * n + r, 24, stride=8), :].astype(bf16)
    for n in range(2):
        rows = coarse[n].astype(f32)
        for r in range(4):
            CB[n, r] = rows[:, r, :].astype(bf16)
    WB[0:9] = outw[...]
    WB[9] = maskw[...]
    pstage[...] = jnp.zeros_like(pstage)
    for j, ref in enumerate((lat_gain, lat_shift, out_gain, out_shift, mask_bias)):
        pstage[j : j + 1, 0:32] = ref[...].astype(f32)
    PB[me] = pstage[...]
    WL[me, core] = latw[core]
    WC[pl.ds(5 * half, 5), me, core] = WB[pl.ds(5 * half, 5), core]
    pl.semaphore_wait(barrier, len(peers))

    latw_c, par_c, w_c = [], [], []
    for k, o in enumerate(CHAN_OFF):
        dev = chan_peer(*o)
        latw_c.append(remote(latw.at[core], WL.at[me, core], s_latw.at[k], r_latw.at[k], dev))
        par_c.append(remote(pstage, PB.at[me], s_par.at[k], r_par.at[k], dev))
        w_c.append(remote(WB.at[pl.ds(5 * half, 5), core], WC.at[pl.ds(5 * half, 5), me, core],
                          s_w.at[k], r_w.at[k], dev))
    for c in latw_c:
        c.start()
    shares = []
    for k, (xh, dc, dl) in enumerate(DEST):
        xd = 2 * core + xh
        dev = (z, yh, dc, xd, dl)
        is_self = (xd == x) & (dc == core) & (dl == yl)
        pos = 2 * xh + dc
        cf = remote(FB.at[dl, pl.ds(2 * pos, 2)], X.at[pl.ds(1, 2), me], s_fine.at[k], r_fine.at[me], dev)
        cc = remote(CB.at[dl, pos], C.at[1, me], s_coarse.at[k], r_coarse.at[me], dev)
        shares.append((is_self, cf, cc))

        @pl.when(is_self)
        def _():
            X[pl.ds(1, 2), me] = FB[dl, pl.ds(2 * pos, 2)]
            C[1, me] = CB[dl, pos]

        @pl.when(jnp.logical_not(is_self))
        def _():
            cf.start()

    for is_self, _, cc in shares:
        @pl.when(jnp.logical_not(is_self))
        def _():
            cc.start()

    for c in w_c:
        c.start()
    for c in par_c:
        c.start()

    def wait_shares(buf, width, send, recv):
        for s in range(8):
            @pl.when(jnp.logical_not((s == me) & (lax.div(x, 2) == core)))
            def _():
                dst = buf.at[pl.ds(1, width), s]
                remote(dst, dst, send.at[s], recv.at[s], partner).wait_recv()

    ci = lax.broadcasted_iota(jnp.int32, (256, COLS), 0)
    cj = lax.broadcasted_iota(jnp.int32, (256, COLS), 1)
    center = lax.shift_right_logical(cj, 1)
    side = jnp.clip(jnp.where(lax.bitwise_and(cj, 1) == 0, center - 1, center + 1), 0, 255)
    widen = (jnp.where(ci == center, 0.75, 0.0) + jnp.where(ci == side, 0.25, 0.0)).astype(bf16)

    def lateral_of(slot):
        rows = X[slot].astype(f32).reshape(192, COLS).astype(bf16)
        return jnp.dot(WL[...].reshape(256, 192), rows, preferred_element_type=f32)

    def row_stats(rows):
        s = q = None
        for row in rows:
            for k in range(COLS // 128):
                t = row[:, 128 * k : 128 * (k + 1)]
                s = t if s is None else s + t
                q = t * t if q is None else q + t * t
        both = jnp.concatenate(
            [jnp.sum(s.reshape(GROUPS, 8, 128), 1), jnp.sum(q.reshape(GROUPS, 8, 128), 1),
             jnp.zeros((64, 128), f32)], 0)
        return jnp.sum(jnp.transpose(both), 0, keepdims=True)

    def scale_shift(total, gain, shift):
        tall = jnp.transpose(jnp.broadcast_to(total, (128, 128)))
        mean = tall[0:32] / pixels
        var = tall[32:64] / pixels - mean * mean
        rstd = lax.rsqrt(var + epsilon)
        spread = lambda v: jnp.broadcast_to(v[:, None, :], (GROUPS, 8, 128)).reshape(D, 128)
        a = spread(rstd) * gain
        return a, shift - spread(mean) * a

    def send_plane(it, offsets):
        done = []
        for k, o in enumerate(PLANE_OFF):
            if o in offsets:
                c = remote(plane_src.at[it], plane_dst.at[it, k], s_plane.at[it, k],
                           r_plane.at[it, k], plane_peer(*o))
                c.start()
                done.append(c)
        return done

    def send_line(it):
        done = []
        for k, o in enumerate(LINE_OFF):
            c = remote(line_src.at[it], line_dst.at[it, k], s_line.at[it, k],
                       r_line.at[it, k], line_peer(*o))
            c.start()
            done.append(c)
        return done

    def line_total(it):
        t = line_src[it]
        for k in range(len(LINE_OFF)):
            t = t + line_dst[it, k]
        return t

    for c in latw_c:
        c.wait_recv()
    latw_core = remote(WL.at[:, core], WL.at[:, core], s_core.at[0], r_core.at[0], partner)
    latw_core.start()
    wait_shares(X, 2, s_fine, r_fine)
    latw_core.wait_recv()
    own_rows = [lateral_of(1), lateral_of(2)]
    LAT[1] = own_rows[0]
    LAT[2] = own_rows[1]
    line_src[0] = jnp.concatenate([row_stats(own_rows), jnp.zeros((1, 128), f32)], 0)
    line1 = send_line(0)

    halo_c = [
        remote(X.at[1], X.at[3], s_halo.at[0], r_halo.at[0], above),
        remote(X.at[2], X.at[0], s_halo.at[1], r_halo.at[1], below),
    ]
    for c in halo_c:
        c.start()
    wait_shares(C, 1, s_coarse, r_coarse)
    coarse_halo = [
        remote(C.at[1], C.at[2], s_halo.at[2], r_halo.at[2], above),
        remote(C.at[1], C.at[0], s_halo.at[3], r_halo.at[3], below),
    ]
    for c in coarse_halo:
        c.start()

    for c in line1:
        c.wait_recv()
    plane_src[0] = line_total(0)[0:1]
    plane1 = send_plane(0, SAME_OFF)

    for c in w_c:
        c.wait_recv()
    mine = pl.ds(5 * half, 5)
    yours = pl.ds(5 * (1 - half), 5)
    lower = WC.at[mine, pl.ds(0, 4), core]
    upper = WC.at[mine, pl.ds(4, 4), core]
    z_c = [
        remote(lower, lower, s_z.at[0], r_z.at[0], line_peer(1, 0)),
        remote(upper, upper, s_z.at[1], r_z.at[1], line_peer(7, 0)),
    ]
    for c in z_c:
        c.start()
    core_c = [remote(WC.at[mine, :, core], WC.at[mine, :, core], s_core.at[1], r_core.at[1], partner)]
    core_c[0].start()

    for c in par_c:
        c.wait_recv()
    turned = jnp.transpose(jnp.concatenate([PB[...].reshape(64, 128), jnp.zeros((64, 128), f32)], 0))

    def param(j):
        col = jnp.concatenate([turned[0:32, 8 * s + j : 8 * s + j + 1] for s in range(8)], 0)
        return jnp.broadcast_to(col, (D, 128))

    for c in halo_c:
        c.wait_recv()
    LAT[0] = lateral_of(0)
    LAT[3] = lateral_of(3)
    for c in coarse_halo:
        c.wait_recv()
    wide = [jnp.dot(C[s].reshape(256, 256), widen, preferred_element_type=f32) for s in range(3)]
    top = jnp.where(pair == 0, wide[1], wide[0])
    bottom = jnp.where(pair == 127, wide[1], wide[2])
    UPS[0] = 0.75 * top + 0.25 * wide[1]
    UPS[1] = 0.25 * top + 0.75 * wide[1]
    UPS[2] = 0.75 * wide[1] + 0.25 * bottom
    UPS[3] = 0.25 * wide[1] + 0.75 * bottom

    your_lower = WC.at[yours, pl.ds(0, 4), core]
    your_upper = WC.at[yours, pl.ds(4, 4), core]
    remote(your_lower, your_lower, s_z.at[0], r_z.at[0], partner).wait_recv()
    remote(your_upper, your_upper, s_z.at[1], r_z.at[1], partner).wait_recv()
    core_c.append(
        remote(WC.at[yours, :, core], WC.at[yours, :, core], s_core.at[2], r_core.at[2], partner)
    )
    core_c[1].start()

    for c in plane1:
        c.wait_recv()
    t = plane_src[0]
    for k, o in enumerate(PLANE_OFF):
        if o in SAME_OFF:
            t = t + plane_dst[0, k]
    a, b = scale_shift(t, param(0), param(1))
    a4 = jnp.concatenate([a] * 4, 1)
    b4 = jnp.concatenate([b] * 4, 1)
    lane = lax.broadcasted_iota(jnp.int32, (D, COLS), 1)
    for s in range(4):
        j = LAT[s] * a4 + b4 + UPS[s]
        if s == 0:
            j = jnp.where(pair == 0, 0.0, j)
        if s == 3:
            j = jnp.where(pair == 127, 0.0, j)
        cols = slice(COLS * s, COLS * (s + 1))
        JS[0:256, cols] = jnp.where(lane == 0, 0.0, pltpu.roll(j, 1, 1)).astype(bf16)
        JS[256:512, cols] = j.astype(bf16)
        JS[512:768, cols] = jnp.where(lane == COLS - 1, 0.0, pltpu.roll(j, COLS - 1, 1)).astype(bf16)

    for part, c in ((mine, core_c[0]), (yours, core_c[1])):
        from_partner = WC.at[part, :, 1 - core]
        remote(from_partner, from_partner, s_core.at[1], r_core.at[1 if c is core_c[0] else 2],
               partner).wait_recv()
    acc = None
    for tap in range(3):
        w = jnp.concatenate([WC[3 * tap + i].reshape(256, 256) for i in range(3)], 1)
        term = jnp.dot(w, JS[:, COLS * tap : COLS * (tap + 2)], preferred_element_type=f32)
        acc = term if acc is None else acc + term
    CO[0] = acc[:, :COLS].astype(bf16)
    CO[1] = acc[:, COLS:].astype(bf16)
    plane_src[1] = row_stats([acc[:, :COLS], acc[:, COLS:]])
    plane2 = send_plane(1, PLANE_OFF)
    xf = lax.rem(2 * x + core, 4)
    kept = (xf == x) & (lax.div(x, 2) == core)
    row_c = []
    for j in range(2):
        is_self = kept & (yl == j)
        c = remote(CO.at[j], R.at[yl], s_row.at[j], r_row.at[yl], (z, yh, lax.div(x, 2), xf, j))
        row_c.append((is_self, c))

        @pl.when(is_self)
        def _():
            R[yl] = CO[j]

        @pl.when(jnp.logical_not(is_self))
        def _():
            c.start()

    for c in plane2:
        c.wait_recv()
    mine_sum, other_sum = plane_src[1], None
    for k, o in enumerate(PLANE_OFF):
        v = plane_dst[1, k]
        if o[2] == 0:
            mine_sum = mine_sum + v
        else:
            other_sum = v if other_sum is None else other_sum + v
    line_src[1] = jnp.concatenate([mine_sum, other_sum], 0)
    line2 = send_line(1)
    gain2, shift2, bias = param(2), param(3), param(4)
    bias4 = jnp.concatenate([bias] * 4, 1)
    for n in range(2):
        @pl.when(jnp.logical_not(kept & (yl == n)))
        def _():
            remote(R.at[n], R.at[n], s_row.at[n], r_row.at[n], partner).wait_recv()

    for c in line2:
        c.wait_recv()
    total = line_total(1)
    mask_w = WC[9].reshape(256, 256)
    for who in range(2):
        image = yl if who == 0 else 1 - yl
        a, b = scale_shift(total[who : who + 1], gain2, shift2)
        act = jnp.maximum(
            R[image].astype(f32) * jnp.concatenate([a] * 4, 1) + jnp.concatenate([b] * 4, 1), 0.0
        ).astype(bf16)
        feat = (jnp.dot(mask_w, act, preferred_element_type=f32) + bias4).astype(bf16)
        logits = jnp.dot(queries[...], feat, preferred_element_type=f32)
        shifted = logits - jnp.max(logits, 0, keepdims=True)
        res = shifted - jnp.log(jnp.sum(jnp.exp(shifted), 0, keepdims=True))
        for k in range(4):
            out[image, pl.ds(k, 200, stride=4), :] = res[:, 128 * k : 128 * (k + 1)]

    for group in (latw_c, par_c, w_c, [latw_core], halo_c, coarse_halo, z_c, core_c, plane1, plane2,
                  line1, line2):
        for c in group:
            c.wait_send()
    for is_self, *cs in shares + row_c:
        @pl.when(jnp.logical_not(is_self))
        def _():
            for c in cs:
                c.wait_send()


def per_device(
    fine_features, coarse_level, lat_weight, lat_gain, lat_shift, out_weight, out_gain, out_shift,
    mask_weight, mask_bias, queries,
):
    pixels = float(D // GROUPS * 256 * COLS)
    vec = lambda v: v.reshape(1, 32)
    V = pltpu.VMEM
    dma = pltpu.SemaphoreType.DMA
    out = pl.pallas_call(
        functools.partial(kernel, pixels),
        out_shape=jax.ShapeDtypeStruct((2, 800, 128), f32),
        in_specs=[pl.BlockSpec(memory_space=V)] * 11,
        out_specs=pl.BlockSpec(memory_space=V),
        scratch_shapes=[
            V((4 * 384, 128), f32),
            V((2, 8, 24, COLS), bf16),
            V((2, 4, 32, 256), bf16),
            V((10, 2, 16, 256), bf16),
            V((4, 8, 24, COLS), bf16),
            V((3, 8, 32, 256), bf16),
            V((8, 2, 16, 192), bf16),
            V((10, 8, 2, 16, 256), bf16),
            V((8, 8, 128), f32),
            V((8, 128), f32),
            V((4, D, COLS), f32),
            V((4, D, COLS), f32),
            V((3 * D, 4 * COLS), bf16),
            V((2, D, COLS), bf16),
            V((2, D, COLS), bf16),
            V((2, 1, 128), f32),
            V((2, 15, 1, 128), f32),
            V((2, 2, 128), f32),
            V((2, 15, 2, 128), f32),
        ]
        + [dma((8,))] * 4
        + [dma((7,))] * 6
        + [dma((4,))] * 2
        + [dma((2,))] * 2
        + [dma((3,))] * 2
        + [dma((2, 15))] * 4
        + [dma((2,))] * 2,
        compiler_params=pltpu.CompilerParams(
            collective_id=0, has_side_effects=True, vmem_limit_bytes=56 * 1024 * 1024
        ),
        name="merge",
    )(
        fine_features.reshape(384, COLS), coarse_level, lat_weight.reshape(2, 16, 192),
        vec(lat_gain), vec(lat_shift),
        out_weight.reshape(9, 2, 16, 256), vec(out_gain), vec(out_shift),
        mask_weight.reshape(2, 16, 256), vec(mask_bias), queries,
    )
    return out.reshape(2, 200, 1, COLS)


def solution(mesh):
    finer = Mesh(mesh.devices.reshape(8, 2, 2, 4, 2), AXES)
    return jax.shard_map(
        per_device,
        mesh=finer,
        in_specs=(
            P(None, CHAN, BAND, None),
            P(None, CHAN, BAND, None),
            P(CHAN, None),
            P(CHAN),
            P(CHAN),
            P(None, None, CHAN, None),
            P(CHAN),
            P(CHAN),
            P(CHAN, None),
            P(CHAN),
            P(),
        ),
        out_specs=P(None, None, AXES, None),
        check_vma=False,
    )
```

```python
import functools

import jax
import jax.numpy as jnp
from jax import lax
from jax.experimental import pallas as pl
from jax.experimental.pallas import tpu as pltpu
from jax.sharding import Mesh
from jax.sharding import PartitionSpec as P

D = 256
GROUPS = 32
COLS = 512
AXES = ("band_0", "band_1", "band_2", "chan_0", "chan_1")
BAND = AXES[:3]
CHAN = AXES[3:]
MESH = pl.DeviceIdType.MESH
f32, bf16 = jnp.float32, jnp.bfloat16
epsilon = 1e-05

CHAN_OFF = [(dx, dy) for dx in (2, 1, 3, 0) for dy in (1, 0) if (dx, dy) != (0, 0)]
PLANE_OFF = [
    (dx, dh, dl)
    for dx in (2, 1, 3, 0)
    for dh in (1, 0)
    for dl in (1, 0)
    if (dx, dh, dl) != (0, 0, 0)
]
SAME_OFF = [o for o in PLANE_OFF if o[1] == o[2]]
LINE_OFF = [(dz, dc) for dz in (4, 3, 5, 2, 6, 1, 7, 0) for dc in (1, 0) if (dz, dc) != (0, 0)]
DEST = [(0, 0, 1), (1, 1, 0), (0, 0, 0), (1, 1, 1), (0, 1, 1), (1, 0, 0), (0, 1, 0), (1, 0, 1)]


def kernel(
    pixels,
    fine_in, coarse_in, latw_in, lat_gain, lat_shift, outw_in, out_gain, out_shift, maskw_in, mask_bias,
    act_out, mask_out, bias_out,
    fine, coarse, latw, PV, s_in,
    FS, FB, CB, WB, X, C, WL, WC, PB, pstage, LAT, UPS, JS, CO, R,
    plane_src, plane_dst, line_src, line_dst,
    s_fine, r_fine, s_coarse, r_coarse, s_latw, r_latw, s_par, r_par, s_w, r_w,
    s_halo, r_halo, s_z, r_z, s_core, r_core, s_plane, r_plane, s_line, r_line, s_row, r_row,
):
    z, yh, core = (lax.axis_index(a) for a in BAND)
    x, yl = (lax.axis_index(a) for a in CHAN)
    me = x * 2 + yl
    fold = lambda v, odd: v + odd * (3 - 2 * v)
    xe = fold(x, yh)
    img = lax.rem(yl + yh, 2)
    pair = (z * 2 + yh) * 8 + xe * 2 + core
    half = lax.rem(z, 2)

    def chan_peer(dx, dy, dc=0):
        return (z, yh, lax.rem(core + dc, 2), lax.rem(x + dx, 4), lax.rem(yl + dy, 2))

    def plane_peer(dx, dh, dl):
        return (z, lax.rem(yh + dh, 2), core, lax.rem(x + dx, 4), lax.rem(yl + dl, 2))

    def line_peer(dz, dc):
        return (lax.rem(z + dz, 8), yh, lax.rem(core + dc, 2), x, yl)

    def pair_owner(g):
        k, p = lax.div(g, 8), lax.rem(g, 8)
        odd = lax.rem(k, 2)
        return (lax.div(k, 2), odd, lax.rem(p, 2), fold(lax.div(p, 2), odd), lax.rem(img + odd, 2))

    above = pair_owner(lax.rem(pair + 127, 128))
    below = pair_owner(lax.rem(pair + 1, 128))
    partner = (z, yh, 1 - core, x, yl)

    def remote(src, dst, send, recv, dev):
        return pltpu.make_async_remote_copy(
            src_ref=src, dst_ref=dst, send_sem=send, recv_sem=recv,
            device_id=dev, device_id_type=MESH,
        )

    barrier = pltpu.get_barrier_semaphore()
    peers = (
        [plane_peer(*o) for o in PLANE_OFF]
        + [line_peer(*o) for o in LINE_OFF]
        + [chan_peer(*o, 1) for o in CHAN_OFF]
        + [above, below]
    )
    for dev in peers:
        pl.semaphore_signal(barrier, inc=1, device_id=dev, device_id_type=MESH)

    loads = [
        pltpu.make_async_copy(src, dst, s_in.at[i])
        for i, (src, dst) in enumerate(
            [(fine_in, fine), (latw_in, latw), (coarse_in, coarse), (outw_in, WB.at[pl.ds(0, 9)]),
             (maskw_in, WB.at[9])]
            + [(v, PV.at[j]) for j, v in enumerate((lat_gain, lat_shift, out_gain, out_shift, mask_bias))]
        )
    ]
    for c in loads:
        c.start()
    loads[0].wait()
    for k in range(4):
        cols = slice(128 * k, 128 * (k + 1))
        FS[384 * k : 384 * (k + 1)] = fine[:, cols].astype(f32)
        for n in range(2):
            for r in range(8):
                FB[n, r, :, cols] = FS[pl.ds(384 * k + 192 * n + r, 24, stride=8), :].astype(bf16)
    for c in loads[1:]:
        c.wait()
    for n in range(2):
        rows = coarse[n].astype(f32)
        for r in range(4):
            CB[n, r] = rows[:, r, :].astype(bf16)
    pstage[...] = jnp.zeros_like(pstage)
    for j in range(5):
        pstage[j : j + 1, 0:32] = PV[j].astype(f32)
    PB[me] = pstage[...]
    WL[me, core] = latw[core]
    WC[pl.ds(5 * half, 5), me, core] = WB[pl.ds(5 * half, 5), core]
    pl.semaphore_wait(barrier, len(peers))

    latw_c, par_c, w_c = [], [], []
    for k, o in enumerate(CHAN_OFF):
        dev = chan_peer(*o)
        latw_c.append(remote(latw.at[core], WL.at[me, core], s_latw.at[k], r_latw.at[k], dev))
        par_c.append(remote(pstage, PB.at[me], s_par.at[k], r_par.at[k], dev))
        w_c.append(remote(WB.at[pl.ds(5 * half, 5), core], WC.at[pl.ds(5 * half, 5), me, core],
                          s_w.at[k], r_w.at[k], dev))
    for c in latw_c:
        c.start()
    shares = []
    for k, (ax, ac, al) in enumerate(DEST):
        xh, dc, dl = lax.rem(x + ax, 2), lax.rem(yl + ac, 2), lax.rem(yl + al, 2)
        xd = fold(2 * core + xh, yh)
        image = lax.rem(dl + yh, 2)
        dev = (z, yh, dc, xd, dl)
        is_self = (xd == x) & (dc == core) & (dl == yl)
        pos = 2 * xh + dc
        cf = remote(FB.at[image, pl.ds(2 * pos, 2)], X.at[pl.ds(1, 2), me], s_fine.at[k], r_fine.at[me], dev)
        cc = remote(CB.at[image, pos], C.at[1, me], s_coarse.at[k], r_coarse.at[me], dev)
        shares.append((is_self, cf, cc))

        @pl.when(is_self)
        def _():
            X[pl.ds(1, 2), me] = FB[image, pl.ds(2 * pos, 2)]
            C[1, me] = CB[image, pos]

        @pl.when(jnp.logical_not(is_self))
        def _():
            cf.start()

    for is_self, _, cc in shares:
        @pl.when(jnp.logical_not(is_self))
        def _():
            cc.start()

    for c in w_c:
        c.start()
    for c in par_c:
        c.start()

    def wait_shares(buf, width, send, recv):
        for s in range(8):
            @pl.when(jnp.logical_not((s == me) & (lax.div(xe, 2) == core)))
            def _():
                dst = buf.at[pl.ds(1, width), s]
                remote(dst, dst, send.at[s], recv.at[s], partner).wait_recv()

    ci = lax.broadcasted_iota(jnp.int32, (256, COLS), 0)
    cj = lax.broadcasted_iota(jnp.int32, (256, COLS), 1)
    center = lax.shift_right_logical(cj, 1)
    side = jnp.clip(jnp.where(lax.bitwise_and(cj, 1) == 0, center - 1, center + 1), 0, 255)
    widen = (jnp.where(ci == center, 0.75, 0.0) + jnp.where(ci == side, 0.25, 0.0)).astype(bf16)

    def lateral_of(slot):
        rows = X[slot].astype(f32).reshape(192, COLS).astype(bf16)
        return jnp.dot(WL[...].reshape(256, 192), rows, preferred_element_type=f32)

    def row_stats(rows):
        s = q = None
        for row in rows:
            for k in range(COLS // 128):
                t = row[:, 128 * k : 128 * (k + 1)]
                s = t if s is None else s + t
                q = t * t if q is None else q + t * t
        both = jnp.concatenate(
            [jnp.sum(s.reshape(GROUPS, 8, 128), 1), jnp.sum(q.reshape(GROUPS, 8, 128), 1),
             jnp.zeros((64, 128), f32)], 0)
        return jnp.sum(jnp.transpose(both), 0, keepdims=True)

    def scale_shift(total, gain, shift):
        tall = jnp.transpose(jnp.broadcast_to(total, (128, 128)))
        mean = tall[0:32] / pixels
        var = tall[32:64] / pixels - mean * mean
        rstd = lax.rsqrt(var + epsilon)
        spread = lambda v: jnp.broadcast_to(v[:, None, :], (GROUPS, 8, 128)).reshape(D, 128)
        a = spread(rstd) * gain
        return a, shift - spread(mean) * a

    def send_plane(it, offsets):
        done = []
        for k, o in enumerate(PLANE_OFF):
            if o in offsets:
                c = remote(plane_src.at[it], plane_dst.at[it, k], s_plane.at[it, k],
                           r_plane.at[it, k], plane_peer(*o))
                c.start()
                done.append(c)
        return done

    def send_line(it):
        done = []
        for k, o in enumerate(LINE_OFF):
            c = remote(line_src.at[it], line_dst.at[it, k], s_line.at[it, k],
                       r_line.at[it, k], line_peer(*o))
            c.start()
            done.append(c)
        return done

    def line_total(it):
        t = line_src[it]
        for k in range(len(LINE_OFF)):
            t = t + line_dst[it, k]
        return t

    for c in latw_c:
        c.wait_recv()
    latw_core = remote(WL.at[:, core], WL.at[:, core], s_core.at[0], r_core.at[0], partner)
    latw_core.start()
    wait_shares(X, 2, s_fine, r_fine)
    latw_core.wait_recv()
    own_rows = [lateral_of(1), lateral_of(2)]
    LAT[1] = own_rows[0]
    LAT[2] = own_rows[1]
    line_src[0] = row_stats(own_rows)
    line1 = send_line(0)

    halo_c = [
        remote(X.at[1], X.at[3], s_halo.at[0], r_halo.at[0], above),
        remote(X.at[2], X.at[0], s_halo.at[1], r_halo.at[1], below),
    ]
    for c in halo_c:
        c.start()
    wait_shares(C, 1, s_coarse, r_coarse)
    coarse_halo = [
        remote(C.at[1], C.at[2], s_halo.at[2], r_halo.at[2], above),
        remote(C.at[1], C.at[0], s_halo.at[3], r_halo.at[3], below),
    ]
    for c in coarse_halo:
        c.start()

    for c in w_c:
        c.wait_recv()
    mine = pl.ds(5 * half, 5)
    yours = pl.ds(5 * (1 - half), 5)
    lower = WC.at[mine, pl.ds(0, 4), core]
    upper = WC.at[mine, pl.ds(4, 4), core]
    z_c = [
        remote(lower, lower, s_z.at[0], r_z.at[0], line_peer(1, 0)),
        remote(upper, upper, s_z.at[1], r_z.at[1], line_peer(7, 0)),
    ]
    for c in z_c:
        c.start()
    core_c = [remote(WC.at[mine, :, core], WC.at[mine, :, core], s_core.at[1], r_core.at[1], partner)]
    core_c[0].start()

    for c in line1:
        c.wait_recv()
    plane_src[0] = line_total(0)
    plane1 = send_plane(0, SAME_OFF)

    for c in par_c:
        c.wait_recv()
    turned = jnp.transpose(jnp.concatenate([PB[...].reshape(64, 128), jnp.zeros((64, 128), f32)], 0))

    def param(j):
        col = jnp.concatenate([turned[0:32, 8 * s + j : 8 * s + j + 1] for s in range(8)], 0)
        return jnp.broadcast_to(col, (D, 128))

    for c in halo_c:
        c.wait_recv()
    LAT[0] = lateral_of(0)
    LAT[3] = lateral_of(3)
    for c in coarse_halo:
        c.wait_recv()
    wide = [jnp.dot(C[s].reshape(256, 256), widen, preferred_element_type=f32) for s in range(3)]
    top = jnp.where(pair == 0, wide[1], wide[0])
    bottom = jnp.where(pair == 127, wide[1], wide[2])
    UPS[0] = 0.75 * top + 0.25 * wide[1]
    UPS[1] = 0.25 * top + 0.75 * wide[1]
    UPS[2] = 0.75 * wide[1] + 0.25 * bottom
    UPS[3] = 0.25 * wide[1] + 0.75 * bottom

    your_lower = WC.at[yours, pl.ds(0, 4), core]
    your_upper = WC.at[yours, pl.ds(4, 4), core]
    remote(your_lower, your_lower, s_z.at[0], r_z.at[0], partner).wait_recv()
    remote(your_upper, your_upper, s_z.at[1], r_z.at[1], partner).wait_recv()
    core_c.append(
        remote(WC.at[yours, :, core], WC.at[yours, :, core], s_core.at[2], r_core.at[2], partner)
    )
    core_c[1].start()

    for c in plane1:
        c.wait_recv()
    t = plane_src[0]
    for k, o in enumerate(PLANE_OFF):
        if o in SAME_OFF:
            t = t + plane_dst[0, k]
    a, b = scale_shift(t, param(0), param(1))
    a4 = jnp.concatenate([a] * 4, 1)
    b4 = jnp.concatenate([b] * 4, 1)
    lane = lax.broadcasted_iota(jnp.int32, (D, COLS), 1)
    for s in range(4):
        j = LAT[s] * a4 + b4 + UPS[s]
        if s == 0:
            j = jnp.where(pair == 0, 0.0, j)
        if s == 3:
            j = jnp.where(pair == 127, 0.0, j)
        cols = slice(COLS * s, COLS * (s + 1))
        JS[0:256, cols] = jnp.where(lane == 0, 0.0, pltpu.roll(j, 1, 1)).astype(bf16)
        JS[256:512, cols] = j.astype(bf16)
        JS[512:768, cols] = jnp.where(lane == COLS - 1, 0.0, pltpu.roll(j, COLS - 1, 1)).astype(bf16)

    for part, c in ((mine, core_c[0]), (yours, core_c[1])):
        from_partner = WC.at[part, :, 1 - core]
        remote(from_partner, from_partner, s_core.at[1], r_core.at[1 if c is core_c[0] else 2],
               partner).wait_recv()
    acc = None
    for tap in range(3):
        w = jnp.concatenate([WC[3 * tap + i].reshape(256, 256) for i in range(3)], 1)
        term = jnp.dot(w, JS[:, COLS * tap : COLS * (tap + 2)], preferred_element_type=f32)
        acc = term if acc is None else acc + term
    CO[0] = acc[:, :COLS].astype(bf16)
    CO[1] = acc[:, COLS:].astype(bf16)
    line_src[1] = row_stats([acc[:, :COLS], acc[:, COLS:]])
    line2 = send_line(1)
    xf = lax.rem(2 * xe + core, 4)
    kept = (xf == x) & (lax.div(xe, 2) == core)
    row_c = []
    for j in range(2):
        is_self = kept & (yl == j)
        c = remote(CO.at[j], R.at[img], s_row.at[j], r_row.at[img], (z, yh, lax.div(xe, 2), xf, j))
        row_c.append((is_self, c))

        @pl.when(is_self)
        def _():
            R[img] = CO[j]

        @pl.when(jnp.logical_not(is_self))
        def _():
            c.start()

    gain2, shift2, bias = param(2), param(3), param(4)
    bias_out[...] = bias
    mask_out[...] = WC[9].reshape(256, 256)
    for c in line2:
        c.wait_recv()
    plane_src[1] = line_total(1)
    plane2 = send_plane(1, PLANE_OFF)
    for n in range(2):
        @pl.when(jnp.logical_not(kept & (img == n)))
        def _():
            remote(R.at[n], R.at[n], s_row.at[n], r_row.at[n], partner).wait_recv()

    for c in plane2:
        c.wait_recv()
    mine_sum, other_sum = plane_src[1], None
    for k, o in enumerate(PLANE_OFF):
        v = plane_dst[1, k]
        if o in SAME_OFF:
            mine_sum = mine_sum + v
        else:
            other_sum = v if other_sum is None else other_sum + v
    for image, total in ((img, mine_sum), (1 - img, other_sum)):
        a, b = scale_shift(total, gain2, shift2)
        act_out[image] = jnp.maximum(
            R[image].astype(f32) * jnp.concatenate([a] * 4, 1) + jnp.concatenate([b] * 4, 1), 0.0
        ).astype(bf16)
    for group in (latw_c, par_c, w_c, [latw_core], halo_c, coarse_halo, z_c, core_c, plane1, plane2,
                  line1, line2):
        for c in group:
            c.wait_send()
    for is_self, *cs in shares + row_c:
        @pl.when(jnp.logical_not(is_self))
        def _():
            for c in cs:
                c.wait_send()


def log_probs_of(act, mask_w, bias, queries, out):
    bias4 = jnp.concatenate([bias[...]] * 4, 1)
    feat = (jnp.dot(mask_w[...], act[0], preferred_element_type=f32) + bias4).astype(bf16)
    logits = jnp.dot(queries[...], feat, preferred_element_type=f32)
    shifted = logits - jnp.max(logits, 0, keepdims=True)
    res = shifted - jnp.log(jnp.sum(jnp.exp(shifted), 0, keepdims=True))
    for k in range(4):
        out[0, pl.ds(k, 200, stride=4), :] = res[:, 128 * k : 128 * (k + 1)]


def per_device(
    fine_features, coarse_level, lat_weight, lat_gain, lat_shift, out_weight, out_gain, out_shift,
    mask_weight, mask_bias, queries,
):
    pixels = float(D // GROUPS * 256 * COLS)
    vec = lambda v: v.reshape(1, 32)
    V = pltpu.VMEM
    dma = pltpu.SemaphoreType.DMA
    hbm = lambda v: pltpu.with_memory_space_constraint(v, pltpu.HBM)
    act, mask_w, bias = pl.pallas_call(
        functools.partial(kernel, pixels),
        out_shape=(
            jax.ShapeDtypeStruct((2, D, COLS), bf16),
            jax.ShapeDtypeStruct((D, D), bf16),
            jax.ShapeDtypeStruct((D, 128), f32),
        ),
        in_specs=[pl.BlockSpec(memory_space=pltpu.HBM)] * 10,
        out_specs=(pl.BlockSpec(memory_space=V),) * 3,
        scratch_shapes=[
            V((384, COLS), bf16),
            V((2, 32, 4, 256), bf16),
            V((2, 16, 192), bf16),
            V((5, 1, 32), bf16),
            dma((10,)),
            V((4 * 384, 128), f32),
            V((2, 8, 24, COLS), bf16),
            V((2, 4, 32, 256), bf16),
            V((10, 2, 16, 256), bf16),
            V((4, 8, 24, COLS), bf16),
            V((3, 8, 32, 256), bf16),
            V((8, 2, 16, 192), bf16),
            V((10, 8, 2, 16, 256), bf16),
            V((8, 8, 128), f32),
            V((8, 128), f32),
            V((4, D, COLS), f32),
            V((4, D, COLS), f32),
            V((3 * D, 4 * COLS), bf16),
            V((2, D, COLS), bf16),
            V((2, D, COLS), bf16),
            V((2, 1, 128), f32),
            V((2, 15, 1, 128), f32),
            V((2, 1, 128), f32),
            V((2, 15, 1, 128), f32),
        ]
        + [dma((8,))] * 4
        + [dma((7,))] * 6
        + [dma((4,))] * 2
        + [dma((2,))] * 2
        + [dma((3,))] * 2
        + [dma((2, 15))] * 4
        + [dma((2,))] * 2,
        compiler_params=pltpu.CompilerParams(
            collective_id=0, has_side_effects=True, vmem_limit_bytes=40 * 1024 * 1024
        ),
        name="merge",
    )(*map(hbm, (
        fine_features.reshape(384, COLS), coarse_level, lat_weight.reshape(2, 16, 192),
        vec(lat_gain), vec(lat_shift),
        out_weight.reshape(9, 2, 16, 256), vec(out_gain), vec(out_shift),
        mask_weight.reshape(2, 16, 256), vec(mask_bias),
    )))
    out = pl.pallas_call(
        log_probs_of,
        out_shape=jax.ShapeDtypeStruct((2, 800, 128), f32),
        grid=(2,),
        in_specs=[
            pl.BlockSpec((1, D, COLS), lambda n: (n, 0, 0)),
            pl.BlockSpec((D, D), lambda n: (0, 0)),
            pl.BlockSpec((D, 128), lambda n: (0, 0)),
            pl.BlockSpec((200, D), lambda n: (0, 0)),
        ],
        out_specs=pl.BlockSpec((1, 800, 128), lambda n: (n, 0, 0)),
        compiler_params=pltpu.CompilerParams(vmem_limit_bytes=16 * 1024 * 1024),
        name="log_probs",
    )(act, mask_w, bias, queries)
    return out.reshape(2, 200, 1, COLS)


def solution(mesh):
    finer = Mesh(mesh.devices.reshape(8, 2, 2, 4, 2), AXES)
    return jax.shard_map(
        per_device,
        mesh=finer,
        in_specs=(
            P(None, CHAN, BAND, None),
            P(None, CHAN, BAND, None),
            P(CHAN, None),
            P(CHAN),
            P(CHAN),
            P(None, None, CHAN, None),
            P(CHAN),
            P(CHAN),
            P(CHAN, None),
            P(CHAN),
            P(),
        ),
        out_specs=P(None, None, AXES, None),
        check_vma=False,
    )
```

```python
import functools

import jax
import jax.numpy as jnp
from jax import lax
from jax.experimental import pallas as pl
from jax.experimental.pallas import tpu as pltpu
from jax.sharding import Mesh
from jax.sharding import PartitionSpec as P

D = 256
GROUPS = 32
COLS = 512
AXES = ("band_0", "band_1", "band_2", "chan_0", "chan_1")
BAND = AXES[:3]
CHAN = AXES[3:]
MESH = pl.DeviceIdType.MESH
f32, bf16 = jnp.float32, jnp.bfloat16
epsilon = 1e-05

CHAN_OFF = [(dx, dy) for dx in (2, 1, 3, 0) for dy in (1, 0) if (dx, dy) != (0, 0)]
PLANE_OFF = [
    (dx, dh, dl)
    for dx in (2, 1, 3, 0)
    for dh in (1, 0)
    for dl in (1, 0)
    if (dx, dh, dl) != (0, 0, 0)
]
SAME_OFF = [o for o in PLANE_OFF if o[1] == o[2]]
LINE_OFF = [(dz, dc) for dz in (4, 3, 5, 2, 6, 1, 7, 0) for dc in (1, 0) if (dz, dc) != (0, 0)]
DEST = [(0, 0, 1), (1, 1, 0), (0, 0, 0), (1, 1, 1), (0, 1, 1), (1, 0, 0), (0, 1, 0), (1, 0, 1)]


def kernel(
    pixels,
    fine_in, coarse_in, latw_in, lat_gain, lat_shift, outw_in, out_gain, out_shift, maskw_in, mask_bias,
    act_out, mask_out, bias_out,
    fine, coarse, latw, PV, s_in,
    FS, FB, CB, WB, X, C, WL, WC, PB, pstage, LAT, UPS, JS, CO, R,
    plane_src, plane_dst, line_src, line_dst, line_src2, line_dst2,
    s_fine, r_fine, s_coarse, r_coarse, s_latw, r_latw, s_par, r_par, s_w, r_w,
    s_halo, r_halo, s_z, r_z, s_core, r_core, s_plane, r_plane, s_line, r_line, s_row, r_row,
):
    z, yh, core = (lax.axis_index(a) for a in BAND)
    x, yl = (lax.axis_index(a) for a in CHAN)
    me = x * 2 + yl
    fold = lambda v, odd: v + odd * (3 - 2 * v)
    xe = fold(x, yh)
    img = lax.rem(yl + yh, 2)
    pair = (z * 2 + yh) * 8 + xe * 2 + core
    half = lax.rem(z, 2)

    def chan_peer(dx, dy, dc=0):
        return (z, yh, lax.rem(core + dc, 2), lax.rem(x + dx, 4), lax.rem(yl + dy, 2))

    def plane_peer(dx, dh, dl):
        return (z, lax.rem(yh + dh, 2), core, lax.rem(x + dx, 4), lax.rem(yl + dl, 2))

    def line_peer(dz, dc):
        return (lax.rem(z + dz, 8), yh, lax.rem(core + dc, 2), x, yl)

    def pair_owner(g):
        k, p = lax.div(g, 8), lax.rem(g, 8)
        odd = lax.rem(k, 2)
        return (lax.div(k, 2), odd, lax.rem(p, 2), fold(lax.div(p, 2), odd), lax.rem(img + odd, 2))

    above = pair_owner(lax.rem(pair + 127, 128))
    below = pair_owner(lax.rem(pair + 1, 128))
    partner = (z, yh, 1 - core, x, yl)

    def remote(src, dst, send, recv, dev):
        return pltpu.make_async_remote_copy(
            src_ref=src, dst_ref=dst, send_sem=send, recv_sem=recv,
            device_id=dev, device_id_type=MESH,
        )

    barrier = pltpu.get_barrier_semaphore()
    peers = (
        [plane_peer(*o) for o in PLANE_OFF]
        + [line_peer(*o) for o in LINE_OFF]
        + [chan_peer(*o, 1) for o in CHAN_OFF]
        + [above, below]
    )
    for dev in peers:
        pl.semaphore_signal(barrier, inc=1, device_id=dev, device_id_type=MESH)

    loads = [
        pltpu.make_async_copy(src, dst, s_in.at[i])
        for i, (src, dst) in enumerate(
            [(fine_in, fine), (latw_in, latw), (coarse_in, coarse), (outw_in, WB.at[pl.ds(0, 9)]),
             (maskw_in, WB.at[9])]
            + [(v, PV.at[j]) for j, v in enumerate((lat_gain, lat_shift, out_gain, out_shift, mask_bias))]
        )
    ]
    for c in loads:
        c.start()
    loads[0].wait()
    for k in range(4):
        cols = slice(128 * k, 128 * (k + 1))
        FS[384 * k : 384 * (k + 1)] = fine[:, cols].astype(f32)
        for n in range(2):
            for r in range(8):
                FB[n, r, :, cols] = FS[pl.ds(384 * k + 192 * n + r, 24, stride=8), :].astype(bf16)
    loads[1].wait()
    WL[me, core] = latw[core]
    pl.semaphore_wait(barrier, len(peers))

    latw_c, par_c, w_c = [], [], []
    for k, o in enumerate(CHAN_OFF):
        dev = chan_peer(*o)
        latw_c.append(remote(latw.at[core], WL.at[me, core], s_latw.at[k], r_latw.at[k], dev))
        par_c.append(remote(pstage, PB.at[me], s_par.at[k], r_par.at[k], dev))
        w_c.append(remote(WB.at[pl.ds(5 * half, 5), core], WC.at[pl.ds(5 * half, 5), me, core],
                          s_w.at[k], r_w.at[k], dev))
    for c in latw_c:
        c.start()
    shares = []
    for k, (ax, ac, al) in enumerate(DEST):
        xh, dc, dl = lax.rem(x + ax, 2), lax.rem(yl + ac, 2), lax.rem(yl + al, 2)
        xd = fold(2 * core + xh, yh)
        image = lax.rem(dl + yh, 2)
        dev = (z, yh, dc, xd, dl)
        is_self = (xd == x) & (dc == core) & (dl == yl)
        pos = 2 * xh + dc
        cf = remote(FB.at[image, pl.ds(2 * pos, 2)], X.at[pl.ds(1, 2), me], s_fine.at[k], r_fine.at[me], dev)
        cc = remote(CB.at[image, pos], C.at[1, me], s_coarse.at[k], r_coarse.at[me], dev)
        shares.append((is_self, cf, cc, image, pos))

        @pl.when(is_self)
        def _():
            X[pl.ds(1, 2), me] = FB[image, pl.ds(2 * pos, 2)]

        @pl.when(jnp.logical_not(is_self))
        def _():
            cf.start()

    for c in loads[2:]:
        c.wait()
    for n in range(2):
        rows = coarse[n].astype(f32)
        for r in range(4):
            CB[n, r] = rows[:, r, :].astype(bf16)
    pstage[...] = jnp.zeros_like(pstage)
    for j in range(5):
        pstage[j : j + 1, 0:32] = PV[j].astype(f32)
    PB[me] = pstage[...]
    WC[pl.ds(5 * half, 5), me, core] = WB[pl.ds(5 * half, 5), core]
    for is_self, _, cc, image, pos in shares:
        @pl.when(is_self)
        def _():
            C[1, me] = CB[image, pos]

        @pl.when(jnp.logical_not(is_self))
        def _():
            cc.start()

    for c in w_c:
        c.start()
    for c in par_c:
        c.start()

    def wait_shares(buf, width, send, recv):
        for s in range(8):
            @pl.when(jnp.logical_not((s == me) & (lax.div(xe, 2) == core)))
            def _():
                dst = buf.at[pl.ds(1, width), s]
                remote(dst, dst, send.at[s], recv.at[s], partner).wait_recv()

    ci = lax.broadcasted_iota(jnp.int32, (256, COLS), 0)
    cj = lax.broadcasted_iota(jnp.int32, (256, COLS), 1)
    center = lax.shift_right_logical(cj, 1)
    side = jnp.clip(jnp.where(lax.bitwise_and(cj, 1) == 0, center - 1, center + 1), 0, 255)
    widen = (jnp.where(ci == center, 0.75, 0.0) + jnp.where(ci == side, 0.25, 0.0)).astype(bf16)

    def lateral_of(slot):
        rows = X[slot].astype(f32).reshape(192, COLS).astype(bf16)
        return jnp.dot(WL[...].reshape(256, 192), rows, preferred_element_type=f32)

    def row_stats(rows):
        s = q = None
        for row in rows:
            for k in range(COLS // 128):
                t = row[:, 128 * k : 128 * (k + 1)]
                s = t if s is None else s + t
                q = t * t if q is None else q + t * t
        both = jnp.concatenate(
            [jnp.sum(s.reshape(GROUPS, 8, 128), 1), jnp.sum(q.reshape(GROUPS, 8, 128), 1),
             jnp.zeros((64, 128), f32)], 0)
        return jnp.sum(jnp.transpose(both), 0, keepdims=True)

    def scale_shift(total, gain, shift):
        tall = jnp.transpose(jnp.broadcast_to(total, (128, 128)))
        mean = tall[0:32] / pixels
        var = tall[32:64] / pixels - mean * mean
        rstd = lax.rsqrt(var + epsilon)
        spread = lambda v: jnp.broadcast_to(v[:, None, :], (GROUPS, 8, 128)).reshape(D, 128)
        a = spread(rstd) * gain
        return a, shift - spread(mean) * a

    def send_plane(it, offsets):
        done = []
        for k, o in enumerate(PLANE_OFF):
            if o in offsets:
                c = remote(plane_src.at[it], plane_dst.at[it, k], s_plane.at[it, k],
                           r_plane.at[it, k], plane_peer(*o))
                c.start()
                done.append(c)
        return done

    def send_line(it):
        done = []
        for k, o in enumerate(LINE_OFF):
            c = remote(line_src.at[it], line_dst.at[it, k], s_line.at[it, k],
                       r_line.at[it, k], line_peer(*o))
            c.start()
            done.append(c)
        return done

    def line_total(it):
        t = line_src[it]
        for k in range(len(LINE_OFF)):
            t = t + line_dst[it, k]
        return t

    for c in latw_c:
        c.wait_recv()
    latw_core = remote(WL.at[:, core], WL.at[:, core], s_core.at[0], r_core.at[0], partner)
    latw_core.start()
    wait_shares(X, 2, s_fine, r_fine)
    latw_core.wait_recv()
    own_rows = [lateral_of(1), lateral_of(2)]
    LAT[1] = own_rows[0]
    LAT[2] = own_rows[1]
    line_src[0] = row_stats(own_rows)
    line1 = send_line(0)

    halo_c = [
        remote(X.at[1], X.at[3], s_halo.at[0], r_halo.at[0], above),
        remote(X.at[2], X.at[0], s_halo.at[1], r_halo.at[1], below),
    ]
    for c in halo_c:
        c.start()
    wait_shares(C, 1, s_coarse, r_coarse)
    coarse_halo = [
        remote(C.at[1], C.at[2], s_halo.at[2], r_halo.at[2], above),
        remote(C.at[1], C.at[0], s_halo.at[3], r_halo.at[3], below),
    ]
    for c in coarse_halo:
        c.start()

    for c in w_c:
        c.wait_recv()
    mine = pl.ds(5 * half, 5)
    yours = pl.ds(5 * (1 - half), 5)
    z_c = []
    for i in range(4):
        if i == 0:
            dz = 1
        elif i == 1:
            dz = jnp.where((x == 0) & (yh == 1), 7, 1)
        elif i == 2:
            dz = jnp.where((x == 0) & (yh == 0), 1, 7)
        else:
            dz = 7
        piece = WC.at[mine, pl.ds(2 * i, 2), core]
        z_c.append(remote(piece, piece, s_z.at[i], r_z.at[i], line_peer(dz, 0)))
    for c in z_c:
        c.start()
    core_c = [remote(WC.at[mine, :, core], WC.at[mine, :, core], s_core.at[1], r_core.at[1], partner)]
    core_c[0].start()

    for c in line1:
        c.wait_recv()
    plane_src[0] = line_total(0)
    plane1 = send_plane(0, SAME_OFF)

    for c in par_c:
        c.wait_recv()
    turned = jnp.transpose(jnp.concatenate([PB[...].reshape(64, 128), jnp.zeros((64, 128), f32)], 0))

    def param(j):
        col = jnp.concatenate([turned[0:32, 8 * s + j : 8 * s + j + 1] for s in range(8)], 0)
        return jnp.broadcast_to(col, (D, 128))

    for c in halo_c:
        c.wait_recv()
    LAT[0] = lateral_of(0)
    LAT[3] = lateral_of(3)
    for c in coarse_halo:
        c.wait_recv()
    wide = [jnp.dot(C[s].reshape(256, 256), widen, preferred_element_type=f32) for s in range(3)]
    top = jnp.where(pair == 0, wide[1], wide[0])
    bottom = jnp.where(pair == 127, wide[1], wide[2])
    UPS[0] = 0.75 * top + 0.25 * wide[1]
    UPS[1] = 0.25 * top + 0.75 * wide[1]
    UPS[2] = 0.75 * wide[1] + 0.25 * bottom
    UPS[3] = 0.25 * wide[1] + 0.75 * bottom

    for i in range(4):
        piece = WC.at[yours, pl.ds(2 * i, 2), core]
        remote(piece, piece, s_z.at[i], r_z.at[i], partner).wait_recv()
    core_c.append(
        remote(WC.at[yours, :, core], WC.at[yours, :, core], s_core.at[2], r_core.at[2], partner)
    )
    core_c[1].start()

    for c in plane1:
        c.wait_recv()
    t = plane_src[0]
    for k, o in enumerate(PLANE_OFF):
        if o in SAME_OFF:
            t = t + plane_dst[0, k]
    a, b = scale_shift(t, param(0), param(1))
    a4 = jnp.concatenate([a] * 4, 1)
    b4 = jnp.concatenate([b] * 4, 1)
    lane = lax.broadcasted_iota(jnp.int32, (D, COLS), 1)
    for s in range(4):
        j = LAT[s] * a4 + b4 + UPS[s]
        if s == 0:
            j = jnp.where(pair == 0, 0.0, j)
        if s == 3:
            j = jnp.where(pair == 127, 0.0, j)
        cols = slice(COLS * s, COLS * (s + 1))
        JS[0:256, cols] = jnp.where(lane == 0, 0.0, pltpu.roll(j, 1, 1)).astype(bf16)
        JS[256:512, cols] = j.astype(bf16)
        JS[512:768, cols] = jnp.where(lane == COLS - 1, 0.0, pltpu.roll(j, COLS - 1, 1)).astype(bf16)

    for part, c in ((mine, core_c[0]), (yours, core_c[1])):
        from_partner = WC.at[part, :, 1 - core]
        remote(from_partner, from_partner, s_core.at[1], r_core.at[1 if c is core_c[0] else 2],
               partner).wait_recv()
    xf = lax.rem(2 * xe + core, 4)
    kept = (xf == x) & (lax.div(xe, 2) == core)
    taps = [jnp.concatenate([WC[3 * tap + i].reshape(256, 256) for i in range(3)], 1) for tap in range(3)]
    conv_rows, row_c = [], []
    for step in range(2):
        j = 1 - yl if step == 0 else yl
        acc = None
        for tap in range(3):
            cols = pl.ds(pl.multiple_of(COLS * (tap + j), COLS), COLS)
            term = jnp.dot(taps[tap], JS[:, cols], preferred_element_type=f32)
            acc = term if acc is None else acc + term
        conv_rows.append(acc)
        CO[j] = acc.astype(bf16)
        row_c.append(remote(CO.at[j], R.at[img], s_row.at[step], r_row.at[img],
                            (z, yh, lax.div(xe, 2), xf, j)))
    plane_src[1] = row_stats(conv_rows)
    plane2 = send_plane(1, PLANE_OFF)
    row_c[0].start()

    @pl.when(kept)
    def _():
        R[img] = CO[yl]

    @pl.when(jnp.logical_not(kept))
    def _():
        row_c[1].start()

    gain2, shift2, bias = param(2), param(3), param(4)
    bias_out[...] = bias
    mask_out[...] = WC[9].reshape(256, 256)
    for c in plane2:
        c.wait_recv()
    mine_sum, other_sum = plane_src[1], None
    for k, o in enumerate(PLANE_OFF):
        v = plane_dst[1, k]
        if o in SAME_OFF:
            mine_sum = mine_sum + v
        else:
            other_sum = v if other_sum is None else other_sum + v
    line_src2[...] = jnp.concatenate([mine_sum, other_sum], 0)
    line2 = []
    for k, o in enumerate(LINE_OFF):
        c = remote(line_src2, line_dst2.at[k], s_line.at[1, k], r_line.at[1, k], line_peer(*o))
        c.start()
        line2.append(c)
    for group in (latw_c, par_c, w_c, [latw_core], halo_c, coarse_halo, z_c, core_c, plane1, line1, plane2):
        for c in group:
            c.wait_send()
    for is_self, *cs, _, _ in shares:
        @pl.when(jnp.logical_not(is_self))
        def _():
            for c in cs:
                c.wait_send()

    row_c[0].wait_send()

    @pl.when(jnp.logical_not(kept))
    def _():
        row_c[1].wait_send()

    for n in range(2):
        @pl.when(jnp.logical_not(kept & (img == n)))
        def _():
            remote(R.at[n], R.at[n], s_row.at[n], r_row.at[n], partner).wait_recv()

    for c in line2:
        c.wait_recv()
    both = line_src2[...]
    for k in range(len(LINE_OFF)):
        both = both + line_dst2[k]
    for image, total in ((img, both[0:1]), (1 - img, both[1:2])):
        a, b = scale_shift(total, gain2, shift2)
        act_out[image] = jnp.maximum(
            R[image].astype(f32) * jnp.concatenate([a] * 4, 1) + jnp.concatenate([b] * 4, 1), 0.0
        ).astype(bf16)
    for c in line2:
        c.wait_send()


def log_probs_of(act, mask_w, bias, queries, out):
    bias4 = jnp.concatenate([bias[...]] * 4, 1)
    feat = (jnp.dot(mask_w[...], act[0], preferred_element_type=f32) + bias4).astype(bf16)
    logits = jnp.dot(queries[...], feat, preferred_element_type=f32)
    shifted = logits - jnp.max(logits, 0, keepdims=True)
    res = shifted - jnp.log(jnp.sum(jnp.exp(shifted), 0, keepdims=True))
    for k in range(4):
        out[0, pl.ds(k, 200, stride=4), :] = res[:, 128 * k : 128 * (k + 1)]


def per_device(
    fine_features, coarse_level, lat_weight, lat_gain, lat_shift, out_weight, out_gain, out_shift,
    mask_weight, mask_bias, queries,
):
    pixels = float(D // GROUPS * 256 * COLS)
    vec = lambda v: v.reshape(1, 32)
    V = pltpu.VMEM
    dma = pltpu.SemaphoreType.DMA
    hbm = lambda v: pltpu.with_memory_space_constraint(v, pltpu.HBM)
    act, mask_w, bias = pl.pallas_call(
        functools.partial(kernel, pixels),
        out_shape=(
            jax.ShapeDtypeStruct((2, D, COLS), bf16),
            jax.ShapeDtypeStruct((D, D), bf16),
            jax.ShapeDtypeStruct((D, 128), f32),
        ),
        in_specs=[pl.BlockSpec(memory_space=pltpu.HBM)] * 10,
        out_specs=(pl.BlockSpec(memory_space=V),) * 3,
        scratch_shapes=[
            V((384, COLS), bf16),
            V((2, 32, 4, 256), bf16),
            V((2, 16, 192), bf16),
            V((5, 1, 32), bf16),
            dma((10,)),
            V((4 * 384, 128), f32),
            V((2, 8, 24, COLS), bf16),
            V((2, 4, 32, 256), bf16),
            V((10, 2, 16, 256), bf16),
            V((4, 8, 24, COLS), bf16),
            V((3, 8, 32, 256), bf16),
            V((8, 2, 16, 192), bf16),
            V((10, 8, 2, 16, 256), bf16),
            V((8, 8, 128), f32),
            V((8, 128), f32),
            V((4, D, COLS), f32),
            V((4, D, COLS), f32),
            V((3 * D, 4 * COLS), bf16),
            V((2, D, COLS), bf16),
            V((2, D, COLS), bf16),
            V((2, 1, 128), f32),
            V((2, 15, 1, 128), f32),
            V((1, 1, 128), f32),
            V((1, 15, 1, 128), f32),
            V((2, 128), f32),
            V((15, 2, 128), f32),
        ]
        + [dma((8,))] * 4
        + [dma((7,))] * 6
        + [dma((4,))] * 2
        + [dma((4,))] * 2
        + [dma((3,))] * 2
        + [dma((2, 15))] * 4
        + [dma((2,))] * 2,
        compiler_params=pltpu.CompilerParams(
            collective_id=0, has_side_effects=True, vmem_limit_bytes=40 * 1024 * 1024
        ),
        name="merge",
    )(*map(hbm, (
        fine_features.reshape(384, COLS), coarse_level, lat_weight.reshape(2, 16, 192),
        vec(lat_gain), vec(lat_shift),
        out_weight.reshape(9, 2, 16, 256), vec(out_gain), vec(out_shift),
        mask_weight.reshape(2, 16, 256), vec(mask_bias),
    )))
    out = pl.pallas_call(
        log_probs_of,
        out_shape=jax.ShapeDtypeStruct((2, 800, 128), f32),
        grid=(2,),
        in_specs=[
            pl.BlockSpec((1, D, COLS), lambda n: (n, 0, 0)),
            pl.BlockSpec((D, D), lambda n: (0, 0)),
            pl.BlockSpec((D, 128), lambda n: (0, 0)),
            pl.BlockSpec((200, D), lambda n: (0, 0)),
        ],
        out_specs=pl.BlockSpec((1, 800, 128), lambda n: (n, 0, 0)),
        compiler_params=pltpu.CompilerParams(vmem_limit_bytes=16 * 1024 * 1024),
        name="log_probs",
    )(act, mask_w, bias, queries)
    return out.reshape(2, 200, 1, COLS)


def solution(mesh):
    finer = Mesh(mesh.devices.reshape(8, 2, 2, 4, 2), AXES)
    return jax.shard_map(
        per_device,
        mesh=finer,
        in_specs=(
            P(None, CHAN, BAND, None),
            P(None, CHAN, BAND, None),
            P(CHAN, None),
            P(CHAN),
            P(CHAN),
            P(None, None, CHAN, None),
            P(CHAN),
            P(CHAN),
            P(CHAN, None),
            P(CHAN),
            P(),
        ),
        out_specs=P(None, None, AXES, None),
        check_vma=False,
    )
```

```python
import functools

import jax
import jax.numpy as jnp
from jax import lax
from jax.experimental import pallas as pl
from jax.experimental.pallas import tpu as pltpu
from jax.sharding import Mesh
from jax.sharding import PartitionSpec as P

D = 256
GROUPS = 32
COLS = 512
AXES = ("band_0", "band_1", "band_2", "chan_0", "chan_1")
BAND = AXES[:3]
CHAN = AXES[3:]
MESH = pl.DeviceIdType.MESH
f32, bf16 = jnp.float32, jnp.bfloat16
epsilon = 1e-05

CHAN_OFF = [(dx, dy) for dx in (0, 1, 3, 2) for dy in (1, 0) if (dx, dy) != (0, 0)]
PLANE_OFF = [
    (dx, dh, dl)
    for dx in (2, 1, 3, 0)
    for dh in (1, 0)
    for dl in (1, 0)
    if (dx, dh, dl) != (0, 0, 0)
]
SAME_OFF = [o for o in PLANE_OFF if o[1] == o[2]]
LINE_OFF = [(dz, dc) for dz in (4, 3, 5, 2, 6, 1, 7, 0) for dc in (1, 0) if (dz, dc) != (0, 0)]
DEST = [(0, 0, 1), (1, 1, 0), (0, 0, 0), (1, 1, 1), (0, 1, 1), (1, 0, 0), (0, 1, 0), (1, 0, 1)]
PIECES = (0, 3, 1, 2)


def kernel(
    pixels,
    fine_in, coarse_in, latw_in, lat_gain, lat_shift, outw_in, out_gain, out_shift, maskw_in, mask_bias,
    act_out, mask_out, bias_out,
    fine, coarse, latw, PV, s_in,
    FS, FB, CB, WB, X, C, WL, WC, PB, pstage, LAT, UPS, JS, CO, R,
    plane_src, plane_dst, line_src, line_dst, line_src2, line_dst2,
    s_fine, r_fine, s_coarse, r_coarse, s_latw, r_latw, s_par, r_par, s_w, r_w,
    s_halo, r_halo, s_z, r_z, s_core, r_core, s_plane, r_plane, s_line, r_line, s_row, r_row,
):
    z, yh, core = (lax.axis_index(a) for a in BAND)
    x, yl = (lax.axis_index(a) for a in CHAN)
    me = x * 2 + yl
    fold = lambda v, odd: v + odd * (3 - 2 * v)
    xe = fold(x, yh)
    img = lax.rem(yl + yh, 2)
    pair = (z * 2 + yh) * 8 + xe * 2 + core
    half = lax.rem(z, 2)

    def chan_peer(dx, dy, dc=0):
        return (z, yh, lax.rem(core + dc, 2), lax.rem(x + dx, 4), lax.rem(yl + dy, 2))

    def plane_peer(dx, dh, dl):
        return (z, lax.rem(yh + dh, 2), core, lax.rem(x + dx, 4), lax.rem(yl + dl, 2))

    def line_peer(dz, dc):
        return (lax.rem(z + dz, 8), yh, lax.rem(core + dc, 2), x, yl)

    def pair_owner(g):
        k, p = lax.div(g, 8), lax.rem(g, 8)
        odd = lax.rem(k, 2)
        return (lax.div(k, 2), odd, lax.rem(p, 2), fold(lax.div(p, 2), odd), lax.rem(img + odd, 2))

    above = pair_owner(lax.rem(pair + 127, 128))
    below = pair_owner(lax.rem(pair + 1, 128))
    partner = (z, yh, 1 - core, x, yl)

    def remote(src, dst, send, recv, dev):
        return pltpu.make_async_remote_copy(
            src_ref=src, dst_ref=dst, send_sem=send, recv_sem=recv,
            device_id=dev, device_id_type=MESH,
        )

    barrier = pltpu.get_barrier_semaphore()
    peers = (
        [plane_peer(*o) for o in PLANE_OFF]
        + [line_peer(*o) for o in LINE_OFF]
        + [chan_peer(*o, 1) for o in CHAN_OFF]
        + [above, below]
    )
    for dev in peers:
        pl.semaphore_signal(barrier, inc=1, device_id=dev, device_id_type=MESH)

    loads = [
        pltpu.make_async_copy(src, dst, s_in.at[i])
        for i, (src, dst) in enumerate(
            [(fine_in, fine), (latw_in, latw), (coarse_in, coarse), (outw_in, WB.at[pl.ds(0, 9)]),
             (maskw_in, WB.at[9])]
            + [(v, PV.at[j]) for j, v in enumerate((lat_gain, lat_shift, out_gain, out_shift, mask_bias))]
        )
    ]
    for c in loads:
        c.start()
    loads[0].wait()
    for k in range(4):
        cols = slice(128 * k, 128 * (k + 1))
        FS[384 * k : 384 * (k + 1)] = fine[:, cols].astype(f32)
        for n in range(2):
            for r in range(8):
                FB[n, r, :, cols] = FS[pl.ds(384 * k + 192 * n + r, 24, stride=8), :].astype(bf16)
    loads[1].wait()
    WL[me, core] = latw[core]
    pl.semaphore_wait(barrier, len(peers))

    latw_c, par_c, w_c = [], [], []
    for k, o in enumerate(CHAN_OFF):
        dev = chan_peer(*o)
        latw_c.append(remote(latw.at[core], WL.at[me, core], s_latw.at[k], r_latw.at[k], dev))
        par_c.append(remote(pstage, PB.at[me], s_par.at[k], r_par.at[k], dev))
        w_c.append(remote(WB.at[pl.ds(5 * half, 5), core], WC.at[pl.ds(5 * half, 5), me, core],
                          s_w.at[k], r_w.at[k], dev))
    for c in latw_c:
        c.start()
    shares = []
    for k, (ax, ac, al) in enumerate(DEST):
        xh, dc, dl = lax.rem(x + ax, 2), lax.rem(yl + ac, 2), lax.rem(yl + al, 2)
        xd = fold(2 * core + xh, yh)
        image = lax.rem(dl + yh, 2)
        dev = (z, yh, dc, xd, dl)
        is_self = (xd == x) & (dc == core) & (dl == yl)
        pos = 2 * xh + dc
        cf = remote(FB.at[image, pl.ds(2 * pos, 2)], X.at[pl.ds(1, 2), me], s_fine.at[k], r_fine.at[me], dev)
        cc = remote(CB.at[image, pos], C.at[1, me], s_coarse.at[k], r_coarse.at[me], dev)
        shares.append((is_self, cf, cc, image, pos))

        @pl.when(is_self)
        def _():
            X[pl.ds(1, 2), me] = FB[image, pl.ds(2 * pos, 2)]

        @pl.when(jnp.logical_not(is_self))
        def _():
            cf.start()

    for c in loads[2:]:
        c.wait()
    for n in range(2):
        rows = coarse[n].astype(f32)
        for r in range(4):
            CB[n, r] = rows[:, r, :].astype(bf16)
    pstage[...] = jnp.zeros_like(pstage)
    for j in range(5):
        pstage[j : j + 1, 0:32] = PV[j].astype(f32)
    PB[me] = pstage[...]
    WC[pl.ds(5 * half, 5), me, core] = WB[pl.ds(5 * half, 5), core]
    for is_self, _, cc, image, pos in shares:
        @pl.when(is_self)
        def _():
            C[1, me] = CB[image, pos]

        @pl.when(jnp.logical_not(is_self))
        def _():
            cc.start()


    def wait_shares(buf, width, send, recv):
        for s in range(8):
            @pl.when(jnp.logical_not((s == me) & (lax.div(xe, 2) == core)))
            def _():
                dst = buf.at[pl.ds(1, width), s]
                remote(dst, dst, send.at[s], recv.at[s], partner).wait_recv()

    ci = lax.broadcasted_iota(jnp.int32, (256, COLS), 0)
    cj = lax.broadcasted_iota(jnp.int32, (256, COLS), 1)
    center = lax.shift_right_logical(cj, 1)
    side = jnp.clip(jnp.where(lax.bitwise_and(cj, 1) == 0, center - 1, center + 1), 0, 255)
    widen = (jnp.where(ci == center, 0.75, 0.0) + jnp.where(ci == side, 0.25, 0.0)).astype(bf16)

    def lateral_of(slot):
        rows = X[slot].astype(f32).reshape(192, COLS).astype(bf16)
        return jnp.dot(WL[...].reshape(256, 192), rows, preferred_element_type=f32)

    def row_stats(rows):
        s = q = None
        for row in rows:
            for k in range(COLS // 128):
                t = row[:, 128 * k : 128 * (k + 1)]
                s = t if s is None else s + t
                q = t * t if q is None else q + t * t
        both = jnp.concatenate(
            [jnp.sum(s.reshape(GROUPS, 8, 128), 1), jnp.sum(q.reshape(GROUPS, 8, 128), 1),
             jnp.zeros((64, 128), f32)], 0)
        return jnp.sum(jnp.transpose(both), 0, keepdims=True)

    def scale_shift(total, gain, shift):
        tall = jnp.transpose(jnp.broadcast_to(total, (128, 128)))
        mean = tall[0:32] / pixels
        var = tall[32:64] / pixels - mean * mean
        rstd = lax.rsqrt(var + epsilon)
        spread = lambda v: jnp.broadcast_to(v[:, None, :], (GROUPS, 8, 128)).reshape(D, 128)
        a = spread(rstd) * gain
        return a, shift - spread(mean) * a

    def send_plane(it, offsets):
        done = []
        for k, o in enumerate(PLANE_OFF):
            if o in offsets:
                c = remote(plane_src.at[it], plane_dst.at[it, k], s_plane.at[it, k],
                           r_plane.at[it, k], plane_peer(*o))
                c.start()
                done.append(c)
        return done

    def send_line(it):
        done = []
        for k, o in enumerate(LINE_OFF):
            c = remote(line_src.at[it], line_dst.at[it, k], s_line.at[it, k],
                       r_line.at[it, k], line_peer(*o))
            c.start()
            done.append(c)
        return done

    def line_total(it):
        t = line_src[it]
        for k in range(len(LINE_OFF)):
            t = t + line_dst[it, k]
        return t

    for c in latw_c:
        c.wait_recv()
    latw_core = remote(WL.at[:, core], WL.at[:, core], s_core.at[0], r_core.at[0], partner)
    latw_core.start()
    wait_shares(X, 2, s_fine, r_fine)
    latw_core.wait_recv()
    for c in w_c:
        c.start()
    for c in par_c:
        c.start()
    own_rows = [lateral_of(1), lateral_of(2)]
    LAT[1] = own_rows[0]
    LAT[2] = own_rows[1]
    line_src[0] = row_stats(own_rows)
    line1 = send_line(0)

    halo_c = [
        remote(X.at[1], X.at[3], s_halo.at[0], r_halo.at[0], above),
        remote(X.at[2], X.at[0], s_halo.at[1], r_halo.at[1], below),
    ]
    for c in halo_c:
        c.start()
    wait_shares(C, 1, s_coarse, r_coarse)
    coarse_halo = [
        remote(C.at[1], C.at[2], s_halo.at[2], r_halo.at[2], above),
        remote(C.at[1], C.at[0], s_halo.at[3], r_halo.at[3], below),
    ]
    for c in coarse_halo:
        c.start()

    mine = pl.ds(5 * half, 5)
    yours = pl.ds(5 * (1 - half), 5)
    z_c = []

    def piece_of(part, i):
        return WC.at[part, pl.ds(2 * lax.rem(x + PIECES[i], 4), 2), core]

    def pass_piece(i):
        for k, o in enumerate(CHAN_OFF):
            if (o[0] + PIECES[i]) % 4 == 0:
                w_c[k].wait_recv()
        dz = (1, 7, 1, 7)[i]
        c = remote(piece_of(mine, i), piece_of(mine, i), s_z.at[i], r_z.at[i], line_peer(dz, 0))
        c.start()
        z_c.append(c)

    core_c = []

    def take_piece(i):
        piece = piece_of(yours, i)
        remote(piece, piece, s_z.at[i], r_z.at[i], partner).wait_recv()
        c = remote(piece, piece, s_core.at[2 + i], r_core.at[2 + i], partner)
        c.start()
        core_c.append(c)

    pass_piece(0)
    for c in line1:
        c.wait_recv()
    plane_src[0] = line_total(0)
    plane1 = send_plane(0, SAME_OFF)

    pass_piece(1)
    pass_piece(2)
    pass_piece(3)
    core_mine = remote(WC.at[mine, :, core], WC.at[mine, :, core], s_core.at[1], r_core.at[1], partner)
    core_mine.start()

    for c in par_c:
        c.wait_recv()
    turned = jnp.transpose(jnp.concatenate([PB[...].reshape(64, 128), jnp.zeros((64, 128), f32)], 0))

    def param(j):
        col = jnp.concatenate([turned[0:32, 8 * s + j : 8 * s + j + 1] for s in range(8)], 0)
        return jnp.broadcast_to(col, (D, 128))

    for c in halo_c:
        c.wait_recv()
    LAT[0] = lateral_of(0)
    LAT[3] = lateral_of(3)
    take_piece(0)
    take_piece(1)
    for c in coarse_halo:
        c.wait_recv()
    wide = [jnp.dot(C[s].reshape(256, 256), widen, preferred_element_type=f32) for s in range(3)]
    top = jnp.where(pair == 0, wide[1], wide[0])
    bottom = jnp.where(pair == 127, wide[1], wide[2])
    UPS[0] = 0.75 * top + 0.25 * wide[1]
    UPS[1] = 0.25 * top + 0.75 * wide[1]
    UPS[2] = 0.75 * wide[1] + 0.25 * bottom
    UPS[3] = 0.25 * wide[1] + 0.75 * bottom

    take_piece(2)
    take_piece(3)
    for c in plane1:
        c.wait_recv()
    t = plane_src[0]
    for k, o in enumerate(PLANE_OFF):
        if o in SAME_OFF:
            t = t + plane_dst[0, k]
    a, b = scale_shift(t, param(0), param(1))
    a4 = jnp.concatenate([a] * 4, 1)
    b4 = jnp.concatenate([b] * 4, 1)
    lane = lax.broadcasted_iota(jnp.int32, (D, COLS), 1)
    zero = jnp.zeros((), bf16)
    for s in range(4):
        j = LAT[s] * a4 + b4 + UPS[s]
        if s == 0:
            j = jnp.where(pair == 0, 0.0, j)
        if s == 3:
            j = jnp.where(pair == 127, 0.0, j)
        cols = slice(COLS * s, COLS * (s + 1))
        j = j.astype(bf16)
        JS[0:256, cols] = jnp.where(lane == 0, zero, pltpu.roll(j, 1, 1))
        JS[256:512, cols] = j
        JS[512:768, cols] = jnp.where(lane == COLS - 1, zero, pltpu.roll(j, COLS - 1, 1))

    whole = WC.at[mine, :, 1 - core]
    remote(whole, whole, s_core.at[1], r_core.at[1], partner).wait_recv()
    for i in range(4):
        piece = WC.at[yours, pl.ds(2 * lax.rem(x + PIECES[i], 4), 2), 1 - core]
        remote(piece, piece, s_core.at[2 + i], r_core.at[2 + i], partner).wait_recv()
    xf = lax.rem(2 * xe + core, 4)
    kept = (xf == x) & (lax.div(xe, 2) == core)
    taps = [jnp.concatenate([WC[3 * tap + i].reshape(256, 256) for i in range(3)], 1) for tap in range(3)]
    conv_rows, row_c = [], []
    for step in range(2):
        j = 1 - yl if step == 0 else yl
        acc = None
        for tap in range(3):
            cols = pl.ds(pl.multiple_of(COLS * (tap + j), COLS), COLS)
            term = jnp.dot(taps[tap], JS[:, cols], preferred_element_type=f32)
            acc = term if acc is None else acc + term
        conv_rows.append(acc)
        CO[j] = acc.astype(bf16)
        row_c.append(remote(CO.at[j], R.at[img], s_row.at[step], r_row.at[img],
                            (z, yh, lax.div(xe, 2), xf, j)))
    plane_src[1] = row_stats(conv_rows)
    plane2 = send_plane(1, PLANE_OFF)
    row_c[0].start()

    @pl.when(kept)
    def _():
        R[img] = CO[yl]

    @pl.when(jnp.logical_not(kept))
    def _():
        row_c[1].start()

    gain2, shift2, bias = param(2), param(3), param(4)
    bias_out[...] = bias
    mask_out[...] = WC[9].reshape(256, 256)
    for c in plane2:
        c.wait_recv()
    mine_sum, other_sum = plane_src[1], None
    for k, o in enumerate(PLANE_OFF):
        v = plane_dst[1, k]
        if o in SAME_OFF:
            mine_sum = mine_sum + v
        else:
            other_sum = v if other_sum is None else other_sum + v
    line_src2[...] = jnp.concatenate([mine_sum, other_sum], 0)
    line2 = []
    for k, o in enumerate(LINE_OFF):
        c = remote(line_src2, line_dst2.at[k], s_line.at[1, k], r_line.at[1, k], line_peer(*o))
        c.start()
        line2.append(c)
    for group in (latw_c, par_c, w_c, [latw_core], halo_c, coarse_halo, z_c, core_c, [core_mine], plane1, line1, plane2):
        for c in group:
            c.wait_send()
    for is_self, *cs, _, _ in shares:
        @pl.when(jnp.logical_not(is_self))
        def _():
            for c in cs:
                c.wait_send()

    row_c[0].wait_send()

    @pl.when(jnp.logical_not(kept))
    def _():
        row_c[1].wait_send()

    for n in range(2):
        @pl.when(jnp.logical_not(kept & (img == n)))
        def _():
            remote(R.at[n], R.at[n], s_row.at[n], r_row.at[n], partner).wait_recv()

    for c in line2:
        c.wait_recv()
    both = line_src2[...]
    for k in range(len(LINE_OFF)):
        both = both + line_dst2[k]
    for image, total in ((img, both[0:1]), (1 - img, both[1:2])):
        a, b = scale_shift(total, gain2, shift2)
        act_out[image] = jnp.maximum(
            R[image].astype(f32) * jnp.concatenate([a] * 4, 1) + jnp.concatenate([b] * 4, 1), 0.0
        ).astype(bf16)
    for c in line2:
        c.wait_send()


def log_probs_of(act, mask_w, bias, queries, out):
    bias4 = jnp.concatenate([bias[...]] * 4, 1)
    feat = (jnp.dot(mask_w[...], act[0], preferred_element_type=f32) + bias4).astype(bf16)
    logits = jnp.dot(queries[...], feat, preferred_element_type=f32)
    shifted = logits - jnp.max(logits, 0, keepdims=True)
    res = shifted - jnp.log(jnp.sum(jnp.exp(shifted), 0, keepdims=True))
    for k in range(4):
        out[0, pl.ds(k, 200, stride=4), :] = res[:, 128 * k : 128 * (k + 1)]


def per_device(
    fine_features, coarse_level, lat_weight, lat_gain, lat_shift, out_weight, out_gain, out_shift,
    mask_weight, mask_bias, queries,
):
    pixels = float(D // GROUPS * 256 * COLS)
    vec = lambda v: v.reshape(1, 32)
    V = pltpu.VMEM
    dma = pltpu.SemaphoreType.DMA
    hbm = lambda v: pltpu.with_memory_space_constraint(v, pltpu.HBM)
    act, mask_w, bias = pl.pallas_call(
        functools.partial(kernel, pixels),
        out_shape=(
            jax.ShapeDtypeStruct((2, D, COLS), bf16),
            jax.ShapeDtypeStruct((D, D), bf16),
            jax.ShapeDtypeStruct((D, 128), f32),
        ),
        in_specs=[pl.BlockSpec(memory_space=pltpu.HBM)] * 10,
        out_specs=(pl.BlockSpec(memory_space=V),) * 3,
        scratch_shapes=[
            V((384, COLS), bf16),
            V((2, 32, 4, 256), bf16),
            V((2, 16, 192), bf16),
            V((5, 1, 32), bf16),
            dma((10,)),
            V((4 * 384, 128), f32),
            V((2, 8, 24, COLS), bf16),
            V((2, 4, 32, 256), bf16),
            V((10, 2, 16, 256), bf16),
            V((4, 8, 24, COLS), bf16),
            V((3, 8, 32, 256), bf16),
            V((8, 2, 16, 192), bf16),
            V((10, 8, 2, 16, 256), bf16),
            V((8, 8, 128), f32),
            V((8, 128), f32),
            V((4, D, COLS), f32),
            V((4, D, COLS), f32),
            V((3 * D, 4 * COLS), bf16),
            V((2, D, COLS), bf16),
            V((2, D, COLS), bf16),
            V((2, 1, 128), f32),
            V((2, 15, 1, 128), f32),
            V((1, 1, 128), f32),
            V((1, 15, 1, 128), f32),
            V((2, 128), f32),
            V((15, 2, 128), f32),
        ]
        + [dma((8,))] * 4
        + [dma((7,))] * 6
        + [dma((4,))] * 2
        + [dma((4,))] * 2
        + [dma((6,))] * 2
        + [dma((2, 15))] * 4
        + [dma((2,))] * 2,
        compiler_params=pltpu.CompilerParams(
            collective_id=0, has_side_effects=True, vmem_limit_bytes=40 * 1024 * 1024
        ),
        name="merge",
    )(*map(hbm, (
        fine_features.reshape(384, COLS), coarse_level, lat_weight.reshape(2, 16, 192),
        vec(lat_gain), vec(lat_shift),
        out_weight.reshape(9, 2, 16, 256), vec(out_gain), vec(out_shift),
        mask_weight.reshape(2, 16, 256), vec(mask_bias),
    )))
    out = pl.pallas_call(
        log_probs_of,
        out_shape=jax.ShapeDtypeStruct((2, 800, 128), f32),
        grid=(2,),
        in_specs=[
            pl.BlockSpec((1, D, COLS), lambda n: (n, 0, 0)),
            pl.BlockSpec((D, D), lambda n: (0, 0)),
            pl.BlockSpec((D, 128), lambda n: (0, 0)),
            pl.BlockSpec((200, D), lambda n: (0, 0)),
        ],
        out_specs=pl.BlockSpec((1, 800, 128), lambda n: (n, 0, 0)),
        compiler_params=pltpu.CompilerParams(vmem_limit_bytes=16 * 1024 * 1024),
        name="log_probs",
    )(act, mask_w, bias, queries)
    return out.reshape(2, 200, 1, COLS)


def solution(mesh):
    finer = Mesh(mesh.devices.reshape(8, 2, 2, 4, 2), AXES)
    return jax.shard_map(
        per_device,
        mesh=finer,
        in_specs=(
            P(None, CHAN, BAND, None),
            P(None, CHAN, BAND, None),
            P(CHAN, None),
            P(CHAN),
            P(CHAN),
            P(None, None, CHAN, None),
            P(CHAN),
            P(CHAN),
            P(CHAN, None),
            P(CHAN),
            P(),
        ),
        out_specs=P(None, None, AXES, None),
        check_vma=False,
    )
```

```python
import functools

import jax
import jax.numpy as jnp
from jax import lax
from jax.experimental import pallas as pl
from jax.experimental.pallas import tpu as pltpu
from jax.sharding import Mesh
from jax.sharding import PartitionSpec as P

D = 256
GROUPS = 32
COLS = 512
AXES = ("band_0", "band_1", "band_2", "chan_0", "chan_1")
BAND = AXES[:3]
CHAN = AXES[3:]
MESH = pl.DeviceIdType.MESH
f32, bf16 = jnp.float32, jnp.bfloat16
epsilon = 1e-05

CHAN_OFF = [(dx, dy) for dx in (0, 1, 3, 2) for dy in (1, 0) if (dx, dy) != (0, 0)]
PLANE_OFF = [
    (dx, dh, dl)
    for dx in (2, 1, 3, 0)
    for dh in (1, 0)
    for dl in (1, 0)
    if (dx, dh, dl) != (0, 0, 0)
]
SAME_OFF = [o for o in PLANE_OFF if o[1] == o[2]]
LINE_OFF = [(dz, dc) for dz in (4, 3, 5, 2, 6, 1, 7, 0) for dc in (1, 0) if (dz, dc) != (0, 0)]
DEST = [(0, 0, 1), (1, 1, 0), (0, 0, 0), (1, 1, 1), (0, 1, 1), (1, 0, 0), (0, 1, 0), (1, 0, 1)]
PIECES = (0, 3, 1, 2)


def kernel(
    pixels,
    fine_in, coarse_in, latw_in, lat_gain, lat_shift, outw_in, out_gain, out_shift, maskw_in, mask_bias,
    act_out, mask_out, bias_out,
    fine, coarse, latw, PV, s_in,
    FS, FB, CB, WB, X, C, WL, WC, PB, pstage, LAT, UPS, JS, CO, R,
    plane_src, plane_dst, line_src, line_dst, line_src2, line_dst2,
    s_fine, r_fine, s_coarse, r_coarse, s_latw, r_latw, s_par, r_par, s_w, r_w,
    s_halo, r_halo, s_z, r_z, s_core, r_core, s_plane, r_plane, s_line, r_line, s_row, r_row,
):
    z, yh, core = (lax.axis_index(a) for a in BAND)
    x, yl = (lax.axis_index(a) for a in CHAN)
    me = x * 2 + yl
    fold = lambda v, odd: v + odd * (3 - 2 * v)
    xe = fold(x, yh)
    img = lax.rem(yl + yh, 2)
    pair = (z * 2 + yh) * 8 + xe * 2 + core
    half = lax.rem(z + yh, 2)

    def chan_peer(dx, dy, dc=0):
        return (z, yh, lax.rem(core + dc, 2), lax.rem(x + dx, 4), lax.rem(yl + dy, 2))

    def plane_peer(dx, dh, dl):
        return (z, lax.rem(yh + dh, 2), core, lax.rem(x + dx, 4), lax.rem(yl + dl, 2))

    def line_peer(dz, dc):
        return (lax.rem(z + dz, 8), yh, lax.rem(core + dc, 2), x, yl)

    def pair_owner(g):
        k, p = lax.div(g, 8), lax.rem(g, 8)
        odd = lax.rem(k, 2)
        return (lax.div(k, 2), odd, lax.rem(p, 2), fold(lax.div(p, 2), odd), lax.rem(img + odd, 2))

    above = pair_owner(lax.rem(pair + 127, 128))
    below = pair_owner(lax.rem(pair + 1, 128))
    partner = (z, yh, 1 - core, x, yl)

    def remote(src, dst, send, recv, dev):
        return pltpu.make_async_remote_copy(
            src_ref=src, dst_ref=dst, send_sem=send, recv_sem=recv,
            device_id=dev, device_id_type=MESH,
        )

    barrier = pltpu.get_barrier_semaphore()
    peers = (
        [plane_peer(*o) for o in PLANE_OFF]
        + [line_peer(*o) for o in LINE_OFF]
        + [chan_peer(*o, 1) for o in CHAN_OFF]
        + [above, below]
    )
    for dev in peers:
        pl.semaphore_signal(barrier, inc=1, device_id=dev, device_id_type=MESH)

    loads = [
        pltpu.make_async_copy(src, dst, s_in.at[i])
        for i, (src, dst) in enumerate(
            [(fine_in, fine), (latw_in, latw), (coarse_in, coarse), (outw_in, WB.at[pl.ds(0, 9)]),
             (maskw_in, WB.at[9])]
            + [(v, PV.at[j]) for j, v in enumerate((lat_gain, lat_shift, out_gain, out_shift, mask_bias))]
        )
    ]
    for c in loads:
        c.start()
    loads[0].wait()
    for k in range(4):
        cols = slice(128 * k, 128 * (k + 1))
        FS[384 * k : 384 * (k + 1)] = fine[:, cols].astype(f32)
        for n in range(2):
            for r in range(8):
                FB[n, r, :, cols] = FS[pl.ds(384 * k + 192 * n + r, 24, stride=8), :].astype(bf16)
    loads[1].wait()
    WL[me, core] = latw[core]
    pl.semaphore_wait(barrier, len(peers))

    latw_c, par_c, w_c = [], [], []
    for k, o in enumerate(CHAN_OFF):
        dev = chan_peer(*o)
        latw_c.append(remote(latw.at[core], WL.at[me, core], s_latw.at[k], r_latw.at[k], dev))
        par_c.append(remote(pstage, PB.at[me], s_par.at[k], r_par.at[k], dev))
        w_c.append(remote(WB.at[pl.ds(5 * half, 5), core], WC.at[pl.ds(5 * half, 5), me, core],
                          s_w.at[k], r_w.at[k], dev))
    for c in latw_c:
        c.start()
    shares = []
    for k, (ax, ac, al) in enumerate(DEST):
        xh, dc, dl = lax.rem(x + ax, 2), lax.rem(yl + ac, 2), lax.rem(yl + al, 2)
        xd = fold(2 * core + xh, yh)
        image = lax.rem(dl + yh, 2)
        dev = (z, yh, dc, xd, dl)
        is_self = (xd == x) & (dc == core) & (dl == yl)
        pos = 2 * xh + dc
        cf = remote(FB.at[image, pl.ds(2 * pos, 2)], X.at[pl.ds(1, 2), me], s_fine.at[k], r_fine.at[me], dev)
        cc = remote(CB.at[image, pos], C.at[1, me], s_coarse.at[k], r_coarse.at[me], dev)
        shares.append((is_self, cf, cc, image, pos))

        @pl.when(is_self)
        def _():
            X[pl.ds(1, 2), me] = FB[image, pl.ds(2 * pos, 2)]

        @pl.when(jnp.logical_not(is_self))
        def _():
            cf.start()

    for c in loads[2:]:
        c.wait()
    for n in range(2):
        rows = coarse[n].astype(f32)
        for r in range(4):
            CB[n, r] = rows[:, r, :].astype(bf16)
    pstage[...] = jnp.zeros_like(pstage)
    for j in range(5):
        pstage[j : j + 1, 0:32] = PV[j].astype(f32)
    PB[me] = pstage[...]
    WC[pl.ds(5 * half, 5), me, core] = WB[pl.ds(5 * half, 5), core]
    for is_self, _, cc, image, pos in shares:
        @pl.when(is_self)
        def _():
            C[1, me] = CB[image, pos]

        @pl.when(jnp.logical_not(is_self))
        def _():
            cc.start()


    def wait_shares(buf, width, send, recv):
        for s in range(8):
            @pl.when(jnp.logical_not((s == me) & (lax.div(xe, 2) == core)))
            def _():
                dst = buf.at[pl.ds(1, width), s]
                remote(dst, dst, send.at[s], recv.at[s], partner).wait_recv()

    ci = lax.broadcasted_iota(jnp.int32, (256, COLS), 0)
    cj = lax.broadcasted_iota(jnp.int32, (256, COLS), 1)
    center = lax.shift_right_logical(cj, 1)
    side = jnp.clip(jnp.where(lax.bitwise_and(cj, 1) == 0, center - 1, center + 1), 0, 255)
    widen = (jnp.where(ci == center, 0.75, 0.0) + jnp.where(ci == side, 0.25, 0.0)).astype(bf16)

    def lateral_of(slot):
        rows = X[slot].astype(f32).reshape(192, COLS).astype(bf16)
        return jnp.dot(WL[...].reshape(256, 192), rows, preferred_element_type=f32)

    def row_stats(rows):
        s = q = None
        for row in rows:
            for k in range(COLS // 128):
                t = row[:, 128 * k : 128 * (k + 1)]
                s = t if s is None else s + t
                q = t * t if q is None else q + t * t
        both = jnp.concatenate(
            [jnp.sum(s.reshape(GROUPS, 8, 128), 1), jnp.sum(q.reshape(GROUPS, 8, 128), 1),
             jnp.zeros((64, 128), f32)], 0)
        return jnp.sum(jnp.transpose(both), 0, keepdims=True)

    def scale_shift(total, gain, shift):
        tall = jnp.transpose(jnp.broadcast_to(total, (128, 128)))
        mean = tall[0:32] / pixels
        var = tall[32:64] / pixels - mean * mean
        rstd = lax.rsqrt(var + epsilon)
        spread = lambda v: jnp.broadcast_to(v[:, None, :], (GROUPS, 8, 128)).reshape(D, 128)
        a = spread(rstd) * gain
        return a, shift - spread(mean) * a

    def send_plane(it, offsets):
        done = []
        for k, o in enumerate(PLANE_OFF):
            if o in offsets:
                c = remote(plane_src.at[it], plane_dst.at[it, k], s_plane.at[it, k],
                           r_plane.at[it, k], plane_peer(*o))
                c.start()
                done.append(c)
        return done

    def send_line(it):
        done = []
        for k, o in enumerate(LINE_OFF):
            c = remote(line_src.at[it], line_dst.at[it, k], s_line.at[it, k],
                       r_line.at[it, k], line_peer(*o))
            c.start()
            done.append(c)
        return done

    def line_total(it):
        t = line_src[it]
        for k in range(len(LINE_OFF)):
            t = t + line_dst[it, k]
        return t

    for c in latw_c:
        c.wait_recv()
    latw_core = remote(WL.at[:, core], WL.at[:, core], s_core.at[0], r_core.at[0], partner)
    latw_core.start()
    wait_shares(X, 2, s_fine, r_fine)
    latw_core.wait_recv()
    for c in w_c:
        c.start()
    for c in par_c:
        c.start()
    own_rows = [lateral_of(1), lateral_of(2)]
    LAT[1] = own_rows[0]
    LAT[2] = own_rows[1]
    line_src[0] = row_stats(own_rows)
    line1 = send_line(0)

    halo_c = [
        remote(X.at[1], X.at[3], s_halo.at[0], r_halo.at[0], above),
        remote(X.at[2], X.at[0], s_halo.at[1], r_halo.at[1], below),
    ]
    for c in halo_c:
        c.start()
    wait_shares(C, 1, s_coarse, r_coarse)
    coarse_halo = [
        remote(C.at[1], C.at[2], s_halo.at[2], r_halo.at[2], above),
        remote(C.at[1], C.at[0], s_halo.at[3], r_halo.at[3], below),
    ]
    for c in coarse_halo:
        c.start()

    mine = pl.ds(5 * half, 5)
    yours = pl.ds(5 * (1 - half), 5)
    z_c = []

    def piece_of(part, i):
        return WC.at[part, pl.ds(2 * lax.rem(x + PIECES[i], 4), 2), core]

    def pass_piece(i):
        for k, o in enumerate(CHAN_OFF):
            if (o[0] + PIECES[i]) % 4 == 0:
                w_c[k].wait_recv()
        dev = (line_peer(1, 0), line_peer(7, 0), plane_peer(0, 1, 1), line_peer(1 + 6 * yh, 0))[i]
        c = remote(piece_of(mine, i), piece_of(mine, i), s_z.at[i], r_z.at[i], dev)
        c.start()
        z_c.append(c)

    core_c = []

    def take_piece(i):
        piece = piece_of(yours, i)
        remote(piece, piece, s_z.at[i], r_z.at[i], partner).wait_recv()
        c = remote(piece, piece, s_core.at[2 + i], r_core.at[2 + i], partner)
        c.start()
        core_c.append(c)

    pass_piece(0)
    for c in line1:
        c.wait_recv()
    plane_src[0] = line_total(0)
    plane1 = send_plane(0, SAME_OFF)

    pass_piece(1)
    pass_piece(2)
    pass_piece(3)
    core_mine = remote(WC.at[mine, :, core], WC.at[mine, :, core], s_core.at[1], r_core.at[1], partner)
    core_mine.start()

    for c in par_c:
        c.wait_recv()
    turned = jnp.transpose(jnp.concatenate([PB[...].reshape(64, 128), jnp.zeros((64, 128), f32)], 0))

    def param(j):
        col = jnp.concatenate([turned[0:32, 8 * s + j : 8 * s + j + 1] for s in range(8)], 0)
        return jnp.broadcast_to(col, (D, 128))

    for c in halo_c:
        c.wait_recv()
    LAT[0] = lateral_of(0)
    LAT[3] = lateral_of(3)
    take_piece(0)
    take_piece(1)
    for c in coarse_halo:
        c.wait_recv()
    wide = [jnp.dot(C[s].reshape(256, 256), widen, preferred_element_type=f32) for s in range(3)]
    top = jnp.where(pair == 0, wide[1], wide[0])
    bottom = jnp.where(pair == 127, wide[1], wide[2])
    UPS[0] = 0.75 * top + 0.25 * wide[1]
    UPS[1] = 0.25 * top + 0.75 * wide[1]
    UPS[2] = 0.75 * wide[1] + 0.25 * bottom
    UPS[3] = 0.25 * wide[1] + 0.75 * bottom

    take_piece(2)
    take_piece(3)
    for c in plane1:
        c.wait_recv()
    t = plane_src[0]
    for k, o in enumerate(PLANE_OFF):
        if o in SAME_OFF:
            t = t + plane_dst[0, k]
    a, b = scale_shift(t, param(0), param(1))
    a4 = jnp.concatenate([a] * 4, 1)
    b4 = jnp.concatenate([b] * 4, 1)
    lane = lax.broadcasted_iota(jnp.int32, (D, COLS), 1)
    zero = jnp.zeros((), bf16)
    for s in range(4):
        j = LAT[s] * a4 + b4 + UPS[s]
        if s == 0:
            j = jnp.where(pair == 0, 0.0, j)
        if s == 3:
            j = jnp.where(pair == 127, 0.0, j)
        cols = slice(COLS * s, COLS * (s + 1))
        j = j.astype(bf16)
        JS[0:256, cols] = jnp.where(lane == 0, zero, pltpu.roll(j, 1, 1))
        JS[256:512, cols] = j
        JS[512:768, cols] = jnp.where(lane == COLS - 1, zero, pltpu.roll(j, COLS - 1, 1))

    whole = WC.at[mine, :, 1 - core]
    remote(whole, whole, s_core.at[1], r_core.at[1], partner).wait_recv()
    for i in range(4):
        piece = WC.at[yours, pl.ds(2 * lax.rem(x + PIECES[i], 4), 2), 1 - core]
        remote(piece, piece, s_core.at[2 + i], r_core.at[2 + i], partner).wait_recv()
    xf = lax.rem(2 * xe + core, 4)
    kept = (xf == x) & (lax.div(xe, 2) == core)
    taps = [jnp.concatenate([WC[3 * tap + i].reshape(256, 256) for i in range(3)], 1) for tap in range(3)]
    conv_rows, row_c = [], []
    for step in range(2):
        j = 1 - yl if step == 0 else yl
        acc = None
        for tap in range(3):
            cols = pl.ds(pl.multiple_of(COLS * (tap + j), COLS), COLS)
            term = jnp.dot(taps[tap], JS[:, cols], preferred_element_type=f32)
            acc = term if acc is None else acc + term
        conv_rows.append(acc)
        CO[j] = acc.astype(bf16)
        row_c.append(remote(CO.at[j], R.at[img], s_row.at[step], r_row.at[img],
                            (z, yh, lax.div(xe, 2), xf, j)))
    plane_src[1] = row_stats(conv_rows)
    plane2 = send_plane(1, PLANE_OFF)
    row_c[0].start()

    @pl.when(kept)
    def _():
        R[img] = CO[yl]

    @pl.when(jnp.logical_not(kept))
    def _():
        row_c[1].start()

    gain2, shift2, bias = param(2), param(3), param(4)
    bias_out[...] = bias
    mask_out[...] = WC[9].reshape(256, 256)
    for c in plane2:
        c.wait_recv()
    mine_sum, other_sum = plane_src[1], None
    for k, o in enumerate(PLANE_OFF):
        v = plane_dst[1, k]
        if o in SAME_OFF:
            mine_sum = mine_sum + v
        else:
            other_sum = v if other_sum is None else other_sum + v
    line_src2[...] = jnp.concatenate([mine_sum, other_sum], 0)
    line2 = []
    for k, o in enumerate(LINE_OFF):
        c = remote(line_src2, line_dst2.at[k], s_line.at[1, k], r_line.at[1, k], line_peer(*o))
        c.start()
        line2.append(c)
    for group in (latw_c, par_c, w_c, [latw_core], halo_c, coarse_halo, z_c, core_c, [core_mine], plane1, line1, plane2):
        for c in group:
            c.wait_send()
    for is_self, *cs, _, _ in shares:
        @pl.when(jnp.logical_not(is_self))
        def _():
            for c in cs:
                c.wait_send()

    row_c[0].wait_send()

    @pl.when(jnp.logical_not(kept))
    def _():
        row_c[1].wait_send()

    for n in range(2):
        @pl.when(jnp.logical_not(kept & (img == n)))
        def _():
            remote(R.at[n], R.at[n], s_row.at[n], r_row.at[n], partner).wait_recv()

    for c in line2:
        c.wait_recv()
    both = line_src2[...]
    for k in range(len(LINE_OFF)):
        both = both + line_dst2[k]
    for image, total in ((img, both[0:1]), (1 - img, both[1:2])):
        a, b = scale_shift(total, gain2, shift2)
        act_out[image] = jnp.maximum(
            R[image].astype(f32) * jnp.concatenate([a] * 4, 1) + jnp.concatenate([b] * 4, 1), 0.0
        ).astype(bf16)
    for c in line2:
        c.wait_send()


def log_probs_of(act, mask_w, bias, queries, out):
    bias4 = jnp.concatenate([bias[...]] * 4, 1)
    feat = (jnp.dot(mask_w[...], act[0], preferred_element_type=f32) + bias4).astype(bf16)
    logits = jnp.dot(queries[...], feat, preferred_element_type=f32)
    shifted = logits - jnp.max(logits, 0, keepdims=True)
    res = shifted - jnp.log(jnp.sum(jnp.exp(shifted), 0, keepdims=True))
    for k in range(4):
        out[0, pl.ds(k, 200, stride=4), :] = res[:, 128 * k : 128 * (k + 1)]


def per_device(
    fine_features, coarse_level, lat_weight, lat_gain, lat_shift, out_weight, out_gain, out_shift,
    mask_weight, mask_bias, queries,
):
    pixels = float(D // GROUPS * 256 * COLS)
    vec = lambda v: v.reshape(1, 32)
    V = pltpu.VMEM
    dma = pltpu.SemaphoreType.DMA
    hbm = lambda v: pltpu.with_memory_space_constraint(v, pltpu.HBM)
    act, mask_w, bias = pl.pallas_call(
        functools.partial(kernel, pixels),
        out_shape=(
            jax.ShapeDtypeStruct((2, D, COLS), bf16),
            jax.ShapeDtypeStruct((D, D), bf16),
            jax.ShapeDtypeStruct((D, 128), f32),
        ),
        in_specs=[pl.BlockSpec(memory_space=pltpu.HBM)] * 10,
        out_specs=(pl.BlockSpec(memory_space=V),) * 3,
        scratch_shapes=[
            V((384, COLS), bf16),
            V((2, 32, 4, 256), bf16),
            V((2, 16, 192), bf16),
            V((5, 1, 32), bf16),
            dma((10,)),
            V((4 * 384, 128), f32),
            V((2, 8, 24, COLS), bf16),
            V((2, 4, 32, 256), bf16),
            V((10, 2, 16, 256), bf16),
            V((4, 8, 24, COLS), bf16),
            V((3, 8, 32, 256), bf16),
            V((8, 2, 16, 192), bf16),
            V((10, 8, 2, 16, 256), bf16),
            V((8, 8, 128), f32),
            V((8, 128), f32),
            V((4, D, COLS), f32),
            V((4, D, COLS), f32),
            V((3 * D, 4 * COLS), bf16),
            V((2, D, COLS), bf16),
            V((2, D, COLS), bf16),
            V((2, 1, 128), f32),
            V((2, 15, 1, 128), f32),
            V((1, 1, 128), f32),
            V((1, 15, 1, 128), f32),
            V((2, 128), f32),
            V((15, 2, 128), f32),
        ]
        + [dma((8,))] * 4
        + [dma((7,))] * 6
        + [dma((4,))] * 2
        + [dma((4,))] * 2
        + [dma((6,))] * 2
        + [dma((2, 15))] * 4
        + [dma((2,))] * 2,
        compiler_params=pltpu.CompilerParams(
            collective_id=0, has_side_effects=True, vmem_limit_bytes=40 * 1024 * 1024
        ),
        name="merge",
    )(*map(hbm, (
        fine_features.reshape(384, COLS), coarse_level, lat_weight.reshape(2, 16, 192),
        vec(lat_gain), vec(lat_shift),
        out_weight.reshape(9, 2, 16, 256), vec(out_gain), vec(out_shift),
        mask_weight.reshape(2, 16, 256), vec(mask_bias),
    )))
    out = pl.pallas_call(
        log_probs_of,
        out_shape=jax.ShapeDtypeStruct((2, 800, 128), f32),
        grid=(2,),
        in_specs=[
            pl.BlockSpec((1, D, COLS), lambda n: (n, 0, 0)),
            pl.BlockSpec((D, D), lambda n: (0, 0)),
            pl.BlockSpec((D, 128), lambda n: (0, 0)),
            pl.BlockSpec((200, D), lambda n: (0, 0)),
        ],
        out_specs=pl.BlockSpec((1, 800, 128), lambda n: (n, 0, 0)),
        compiler_params=pltpu.CompilerParams(vmem_limit_bytes=16 * 1024 * 1024),
        name="log_probs",
    )(act, mask_w, bias, queries)
    return out.reshape(2, 200, 1, COLS)


def solution(mesh):
    finer = Mesh(mesh.devices.reshape(8, 2, 2, 4, 2), AXES)
    return jax.shard_map(
        per_device,
        mesh=finer,
        in_specs=(
            P(None, CHAN, BAND, None),
            P(None, CHAN, BAND, None),
            P(CHAN, None),
            P(CHAN),
            P(CHAN),
            P(None, None, CHAN, None),
            P(CHAN),
            P(CHAN),
            P(CHAN, None),
            P(CHAN),
            P(),
        ),
        out_specs=P(None, None, AXES, None),
        check_vma=False,
    )
```

```python
import functools

import jax
import jax.numpy as jnp
from jax import lax
from jax.experimental import pallas as pl
from jax.experimental.pallas import tpu as pltpu
from jax.sharding import Mesh
from jax.sharding import PartitionSpec as P

D = 256
GROUPS = 32
COLS = 512
AXES = ("band_0", "band_1", "band_2", "chan_0", "chan_1")
BAND = AXES[:3]
CHAN = AXES[3:]
MESH = pl.DeviceIdType.MESH
f32, bf16 = jnp.float32, jnp.bfloat16
epsilon = 1e-05

CHAN_OFF = [(dx, dy) for dx in (0, 1, 3, 2) for dy in (1, 0) if (dx, dy) != (0, 0)]
PLANE_OFF = [
    (dx, dh, dl)
    for dx in (2, 1, 3, 0)
    for dh in (1, 0)
    for dl in (1, 0)
    if (dx, dh, dl) != (0, 0, 0)
]
SAME_OFF = [o for o in PLANE_OFF if o[1] == o[2]]
LINE_OFF = [(dz, dc) for dz in (4, 3, 5, 2, 6, 1, 7, 0) for dc in (1, 0) if (dz, dc) != (0, 0)]
DEST = [(0, 0, 1), (1, 1, 0), (0, 0, 0), (1, 1, 1), (0, 1, 1), (1, 0, 0), (0, 1, 0), (1, 0, 1)]
PIECES = (0, 3, 1, 2)


def kernel(
    pixels,
    fine_in, coarse_in, latw_in, lat_gain, lat_shift, outw_in, out_gain, out_shift, maskw_in, mask_bias,
    act_out, mask_out, bias_out,
    fine, coarse, latw, PV, s_in,
    FS, FB, CB, WB, X, C, WL, WC, PB, pstage, LAT, UPS, JS, CO, R,
    plane_src, plane_dst, line_src, line_dst, line_src2, line_dst2,
    s_fine, r_fine, s_coarse, r_coarse, s_latw, r_latw, s_par, r_par, s_w, r_w,
    s_halo, r_halo, s_z, r_z, s_core, r_core, s_plane, r_plane, s_line, r_line, s_row, r_row,
):
    z, yh, core = (lax.axis_index(a) for a in BAND)
    x, yl = (lax.axis_index(a) for a in CHAN)
    me = x * 2 + yl
    fold = lambda v, odd: v + odd * (3 - 2 * v)
    xe = fold(x, yh)
    img = lax.rem(yl + yh, 2)
    pair = (z * 2 + yh) * 8 + xe * 2 + core
    half = lax.rem(z + yh, 2)

    def chan_peer(dx, dy, dc=0):
        return (z, yh, lax.rem(core + dc, 2), lax.rem(x + dx, 4), lax.rem(yl + dy, 2))

    def plane_peer(dx, dh, dl):
        return (z, lax.rem(yh + dh, 2), core, lax.rem(x + dx, 4), lax.rem(yl + dl, 2))

    def line_peer(dz, dc):
        return (lax.rem(z + dz, 8), yh, lax.rem(core + dc, 2), x, yl)

    def pair_owner(g):
        k, p = lax.div(g, 8), lax.rem(g, 8)
        odd = lax.rem(k, 2)
        return (lax.div(k, 2), odd, lax.rem(p, 2), fold(lax.div(p, 2), odd), lax.rem(img + odd, 2))

    above = pair_owner(lax.rem(pair + 127, 128))
    below = pair_owner(lax.rem(pair + 1, 128))
    partner = (z, yh, 1 - core, x, yl)

    def remote(src, dst, send, recv, dev):
        return pltpu.make_async_remote_copy(
            src_ref=src, dst_ref=dst, send_sem=send, recv_sem=recv,
            device_id=dev, device_id_type=MESH,
        )

    barrier = pltpu.get_barrier_semaphore()
    peers = (
        [plane_peer(*o) for o in PLANE_OFF]
        + [line_peer(*o) for o in LINE_OFF]
        + [chan_peer(*o, 1) for o in CHAN_OFF]
        + [above, below]
    )
    for dev in peers:
        pl.semaphore_signal(barrier, inc=1, device_id=dev, device_id_type=MESH)

    loads = [
        pltpu.make_async_copy(src, dst, s_in.at[i])
        for i, (src, dst) in enumerate(
            [(fine_in, fine), (latw_in, latw), (coarse_in, coarse), (outw_in, WB.at[pl.ds(0, 9)]),
             (maskw_in, WB.at[9])]
            + [(v, PV.at[j]) for j, v in enumerate((lat_gain, lat_shift, out_gain, out_shift, mask_bias))]
        )
    ]
    for c in loads:
        c.start()
    loads[0].wait()
    for k in range(4):
        cols = slice(128 * k, 128 * (k + 1))
        FS[384 * k : 384 * (k + 1)] = fine[:, cols].astype(f32)
        for n in range(2):
            for r in range(8):
                FB[n, r, :, cols] = FS[pl.ds(384 * k + 192 * n + r, 24, stride=8), :].astype(bf16)
    loads[1].wait()
    WL[me, core] = latw[core]
    pl.semaphore_wait(barrier, len(peers))

    latw_c, par_c, w_c = [], [], []
    for k, o in enumerate(CHAN_OFF):
        dev = chan_peer(*o)
        latw_c.append(remote(latw.at[core], WL.at[me, core], s_latw.at[k], r_latw.at[k], dev))
        par_c.append(remote(pstage, PB.at[me], s_par.at[k], r_par.at[k], dev))
        w_c.append(remote(WB.at[pl.ds(5 * half, 5), core], WC.at[pl.ds(5 * half, 5), me, core],
                          s_w.at[k], r_w.at[k], dev))
    for c in latw_c:
        c.start()
    shares = []
    for k, (ax, ac, al) in enumerate(DEST):
        xh, dc, dl = lax.rem(x + ax, 2), lax.rem(yl + ac, 2), lax.rem(yl + al, 2)
        xd = fold(2 * core + xh, yh)
        image = lax.rem(dl + yh, 2)
        dev = (z, yh, dc, xd, dl)
        is_self = (xd == x) & (dc == core) & (dl == yl)
        pos = 2 * xh + dc
        cf = remote(FB.at[image, pl.ds(2 * pos, 2)], X.at[pl.ds(1, 2), me], s_fine.at[k], r_fine.at[me], dev)
        cc = remote(CB.at[image, pos], C.at[1, me], s_coarse.at[k], r_coarse.at[me], dev)
        shares.append((is_self, cf, cc, image, pos))

        @pl.when(is_self)
        def _():
            X[pl.ds(1, 2), me] = FB[image, pl.ds(2 * pos, 2)]

        @pl.when(jnp.logical_not(is_self))
        def _():
            cf.start()

    for c in loads[2:]:
        c.wait()
    for n in range(2):
        rows = coarse[n].astype(f32)
        for r in range(4):
            CB[n, r] = rows[:, r, :].astype(bf16)
    pstage[...] = jnp.zeros_like(pstage)
    for j in range(5):
        pstage[j : j + 1, 0:32] = PV[j].astype(f32)
    PB[me] = pstage[...]
    WC[pl.ds(5 * half, 5), me, core] = WB[pl.ds(5 * half, 5), core]
    for is_self, _, cc, image, pos in shares:
        @pl.when(is_self)
        def _():
            C[1, me] = CB[image, pos]

        @pl.when(jnp.logical_not(is_self))
        def _():
            cc.start()


    def wait_shares(buf, width, send, recv):
        for s in range(8):
            @pl.when(jnp.logical_not((s == me) & (lax.div(xe, 2) == core)))
            def _():
                dst = buf.at[pl.ds(1, width), s]
                remote(dst, dst, send.at[s], recv.at[s], partner).wait_recv()

    ci = lax.broadcasted_iota(jnp.int32, (256, COLS), 0)
    cj = lax.broadcasted_iota(jnp.int32, (256, COLS), 1)
    center = lax.shift_right_logical(cj, 1)
    side = jnp.clip(jnp.where(lax.bitwise_and(cj, 1) == 0, center - 1, center + 1), 0, 255)
    widen = (jnp.where(ci == center, 0.75, 0.0) + jnp.where(ci == side, 0.25, 0.0)).astype(bf16)

    def lateral_of(slot):
        rows = X[slot].astype(f32).reshape(192, COLS).astype(bf16)
        return jnp.dot(WL[...].reshape(256, 192), rows, preferred_element_type=f32)

    def row_stats(rows):
        s = q = None
        for row in rows:
            for k in range(COLS // 128):
                t = row[:, 128 * k : 128 * (k + 1)]
                s = t if s is None else s + t
                q = t * t if q is None else q + t * t
        both = jnp.concatenate(
            [jnp.sum(s.reshape(GROUPS, 8, 128), 1), jnp.sum(q.reshape(GROUPS, 8, 128), 1),
             jnp.zeros((64, 128), f32)], 0)
        return jnp.sum(jnp.transpose(both), 0, keepdims=True)

    def scale_shift(total, gain, shift):
        tall = jnp.transpose(jnp.broadcast_to(total, (128, 128)))
        mean = tall[0:32] / pixels
        var = tall[32:64] / pixels - mean * mean
        rstd = lax.rsqrt(var + epsilon)
        spread = lambda v: jnp.broadcast_to(v[:, None, :], (GROUPS, 8, 128)).reshape(D, 128)
        a = spread(rstd) * gain
        return a, shift - spread(mean) * a

    def send_plane(it, offsets):
        done = []
        for k, o in enumerate(PLANE_OFF):
            if o in offsets:
                c = remote(plane_src.at[it], plane_dst.at[it, k], s_plane.at[it, k],
                           r_plane.at[it, k], plane_peer(*o))
                c.start()
                done.append(c)
        return done

    def send_line(it):
        done = []
        for k, o in enumerate(LINE_OFF):
            c = remote(line_src.at[it], line_dst.at[it, k], s_line.at[it, k],
                       r_line.at[it, k], line_peer(*o))
            c.start()
            done.append(c)
        return done

    def line_total(it):
        t = line_src[it]
        for k in range(len(LINE_OFF)):
            t = t + line_dst[it, k]
        return t

    for c in latw_c:
        c.wait_recv()
    latw_core = remote(WL.at[:, core], WL.at[:, core], s_core.at[0], r_core.at[0], partner)
    latw_core.start()
    wait_shares(X, 2, s_fine, r_fine)
    latw_core.wait_recv()
    for c in w_c:
        c.start()
    for c in par_c:
        c.start()
    own_rows = [lateral_of(1), lateral_of(2)]
    LAT[1] = own_rows[0]
    LAT[2] = own_rows[1]
    line_src[0] = row_stats(own_rows)
    line1 = send_line(0)

    halo_c = [
        remote(X.at[1], X.at[3], s_halo.at[0], r_halo.at[0], above),
        remote(X.at[2], X.at[0], s_halo.at[1], r_halo.at[1], below),
    ]
    for c in halo_c:
        c.start()
    wait_shares(C, 1, s_coarse, r_coarse)
    coarse_halo = [
        remote(C.at[1], C.at[2], s_halo.at[2], r_halo.at[2], above),
        remote(C.at[1], C.at[0], s_halo.at[3], r_halo.at[3], below),
    ]
    for c in coarse_halo:
        c.start()

    mine = pl.ds(5 * half, 5)
    yours = pl.ds(5 * (1 - half), 5)
    z_c = []

    def piece_of(part, i):
        return WC.at[part, pl.ds(2 * lax.rem(x + PIECES[i], 4), 2), core]

    def pass_piece(i):
        for k, o in enumerate(CHAN_OFF):
            if (o[0] + PIECES[i]) % 4 == 0:
                w_c[k].wait_recv()
        dev = (line_peer(1, 0), line_peer(7, 0), plane_peer(0, 1, 1), line_peer(1 + 6 * yh, 0))[i]
        c = remote(piece_of(mine, i), piece_of(mine, i), s_z.at[i], r_z.at[i], dev)
        c.start()
        z_c.append(c)

    core_c = []

    def take_piece(i):
        piece = piece_of(yours, i)
        remote(piece, piece, s_z.at[i], r_z.at[i], partner).wait_recv()
        c = remote(piece, piece, s_core.at[2 + i], r_core.at[2 + i], partner)
        c.start()
        core_c.append(c)

    pass_piece(0)
    for c in line1:
        c.wait_recv()
    plane_src[0] = line_total(0)
    plane1 = send_plane(0, SAME_OFF)

    pass_piece(1)
    pass_piece(2)
    pass_piece(3)
    core_mine = remote(WC.at[mine, :, core], WC.at[mine, :, core], s_core.at[1], r_core.at[1], partner)
    core_mine.start()

    for c in par_c:
        c.wait_recv()
    turned = jnp.transpose(jnp.concatenate([PB[...].reshape(64, 128), jnp.zeros((64, 128), f32)], 0))

    def param(j):
        col = jnp.concatenate([turned[0:32, 8 * s + j : 8 * s + j + 1] for s in range(8)], 0)
        return jnp.broadcast_to(col, (D, 128))

    for c in halo_c:
        c.wait_recv()
    LAT[0] = lateral_of(0)
    LAT[3] = lateral_of(3)
    take_piece(0)
    take_piece(1)
    for c in coarse_halo:
        c.wait_recv()
    wide = [jnp.dot(C[s].reshape(256, 256), widen, preferred_element_type=f32) for s in range(3)]
    top = jnp.where(pair == 0, wide[1], wide[0])
    bottom = jnp.where(pair == 127, wide[1], wide[2])
    UPS[0] = 0.75 * top + 0.25 * wide[1]
    UPS[1] = 0.25 * top + 0.75 * wide[1]
    UPS[2] = 0.75 * wide[1] + 0.25 * bottom
    UPS[3] = 0.25 * wide[1] + 0.75 * bottom

    take_piece(2)
    take_piece(3)
    for c in plane1:
        c.wait_recv()
    t = plane_src[0]
    for k, o in enumerate(PLANE_OFF):
        if o in SAME_OFF:
            t = t + plane_dst[0, k]
    a, b = scale_shift(t, param(0), param(1))
    a4 = jnp.concatenate([a] * 4, 1)
    b4 = jnp.concatenate([b] * 4, 1)
    lane = lax.broadcasted_iota(jnp.int32, (D, COLS), 1)
    zero = jnp.zeros((), bf16)
    for s in range(4):
        j = LAT[s] * a4 + b4 + UPS[s]
        if s == 0:
            j = jnp.where(pair == 0, 0.0, j)
        if s == 3:
            j = jnp.where(pair == 127, 0.0, j)
        cols = slice(COLS * s, COLS * (s + 1))
        j = j.astype(bf16)
        JS[0:256, cols] = jnp.where(lane == 0, zero, pltpu.roll(j, 1, 1))
        JS[256:512, cols] = j
        JS[512:768, cols] = jnp.where(lane == COLS - 1, zero, pltpu.roll(j, COLS - 1, 1))

    whole = WC.at[mine, :, 1 - core]
    remote(whole, whole, s_core.at[1], r_core.at[1], partner).wait_recv()
    for i in range(4):
        piece = WC.at[yours, pl.ds(2 * lax.rem(x + PIECES[i], 4), 2), 1 - core]
        remote(piece, piece, s_core.at[2 + i], r_core.at[2 + i], partner).wait_recv()
    xf = lax.rem(2 * xe + core, 4)
    kept = (xf == x) & (lax.div(xe, 2) == core)
    taps = [jnp.concatenate([WC[3 * tap + i].reshape(256, 256) for i in range(3)], 1) for tap in range(3)]
    conv_rows, row_c = [], []
    for step in range(2):
        j = 1 - yl if step == 0 else yl
        acc = None
        for tap in range(3):
            cols = pl.ds(pl.multiple_of(COLS * (tap + j), COLS), COLS)
            term = jnp.dot(taps[tap], JS[:, cols], preferred_element_type=f32)
            acc = term if acc is None else acc + term
        conv_rows.append(acc)
        CO[j] = acc.astype(bf16)
        row_c.append(remote(CO.at[j], R.at[img], s_row.at[step], r_row.at[img],
                            (z, yh, lax.div(xe, 2), xf, j)))
    plane_src[1] = row_stats(conv_rows)
    plane2 = send_plane(1, PLANE_OFF)
    row_c[0].start()

    @pl.when(kept)
    def _():
        R[img] = CO[yl]

    @pl.when(jnp.logical_not(kept))
    def _():
        row_c[1].start()

    gain2, shift2, bias = param(2), param(3), param(4)
    bias_out[...] = bias
    mask_out[...] = WC[9].reshape(256, 256)
    for c in plane2:
        c.wait_recv()
    mine_sum, other_sum = plane_src[1], None
    for k, o in enumerate(PLANE_OFF):
        v = plane_dst[1, k]
        if o in SAME_OFF:
            mine_sum = mine_sum + v
        else:
            other_sum = v if other_sum is None else other_sum + v
    line_src2[...] = jnp.concatenate([mine_sum, other_sum], 0)
    line2 = []
    for k, o in enumerate(LINE_OFF):
        c = remote(line_src2, line_dst2.at[k], s_line.at[1, k], r_line.at[1, k], line_peer(*o))
        c.start()
        line2.append(c)
    for group in (latw_c, par_c, w_c, [latw_core], halo_c, coarse_halo, z_c, core_c, [core_mine], plane1, line1, plane2):
        for c in group:
            c.wait_send()
    for is_self, *cs, _, _ in shares:
        @pl.when(jnp.logical_not(is_self))
        def _():
            for c in cs:
                c.wait_send()

    row_c[0].wait_send()

    @pl.when(jnp.logical_not(kept))
    def _():
        row_c[1].wait_send()

    for n in range(2):
        @pl.when(jnp.logical_not(kept & (img == n)))
        def _():
            remote(R.at[n], R.at[n], s_row.at[n], r_row.at[n], partner).wait_recv()

    for c in line2:
        c.wait_recv()
    both = line_src2[...]
    for k in range(len(LINE_OFF)):
        both = both + line_dst2[k]
    for image, total in ((img, both[0:1]), (1 - img, both[1:2])):
        a, b = scale_shift(total, gain2, shift2)
        act_out[image] = jnp.maximum(
            R[image].astype(f32) * jnp.concatenate([a] * 4, 1) + jnp.concatenate([b] * 4, 1), 0.0
        ).astype(bf16)
    for c in line2:
        c.wait_send()


def log_probs_of(act, mask_w, bias, queries, out, buf, sem):
    bias4 = jnp.concatenate([bias[...]] * 4, 1)
    copies = []
    for n in range(2):
        feat = (jnp.dot(mask_w[...], act[n], preferred_element_type=f32) + bias4).astype(bf16)
        logits = jnp.dot(queries[...], feat, preferred_element_type=f32)
        shifted = logits - jnp.max(logits, 0, keepdims=True)
        res = shifted - jnp.log(jnp.sum(jnp.exp(shifted), 0, keepdims=True))
        for k in range(4):
            buf[n, pl.ds(k, 200, stride=4), :] = res[:, 128 * k : 128 * (k + 1)]
        copies.append(pltpu.make_async_copy(buf.at[n], out.at[n], sem.at[n]))
        copies[n].start()
    for c in copies:
        c.wait()


def per_device(
    fine_features, coarse_level, lat_weight, lat_gain, lat_shift, out_weight, out_gain, out_shift,
    mask_weight, mask_bias, queries,
):
    pixels = float(D // GROUPS * 256 * COLS)
    vec = lambda v: v.reshape(1, 32)
    V = pltpu.VMEM
    dma = pltpu.SemaphoreType.DMA
    hbm = lambda v: pltpu.with_memory_space_constraint(v, pltpu.HBM)
    act, mask_w, bias = pl.pallas_call(
        functools.partial(kernel, pixels),
        out_shape=(
            jax.ShapeDtypeStruct((2, D, COLS), bf16),
            jax.ShapeDtypeStruct((D, D), bf16),
            jax.ShapeDtypeStruct((D, 128), f32),
        ),
        in_specs=[pl.BlockSpec(memory_space=pltpu.HBM)] * 10,
        out_specs=(pl.BlockSpec(memory_space=V),) * 3,
        scratch_shapes=[
            V((384, COLS), bf16),
            V((2, 32, 4, 256), bf16),
            V((2, 16, 192), bf16),
            V((5, 1, 32), bf16),
            dma((10,)),
            V((4 * 384, 128), f32),
            V((2, 8, 24, COLS), bf16),
            V((2, 4, 32, 256), bf16),
            V((10, 2, 16, 256), bf16),
            V((4, 8, 24, COLS), bf16),
            V((3, 8, 32, 256), bf16),
            V((8, 2, 16, 192), bf16),
            V((10, 8, 2, 16, 256), bf16),
            V((8, 8, 128), f32),
            V((8, 128), f32),
            V((4, D, COLS), f32),
            V((4, D, COLS), f32),
            V((3 * D, 4 * COLS), bf16),
            V((2, D, COLS), bf16),
            V((2, D, COLS), bf16),
            V((2, 1, 128), f32),
            V((2, 15, 1, 128), f32),
            V((1, 1, 128), f32),
            V((1, 15, 1, 128), f32),
            V((2, 128), f32),
            V((15, 2, 128), f32),
        ]
        + [dma((8,))] * 4
        + [dma((7,))] * 6
        + [dma((4,))] * 2
        + [dma((4,))] * 2
        + [dma((6,))] * 2
        + [dma((2, 15))] * 4
        + [dma((2,))] * 2,
        compiler_params=pltpu.CompilerParams(
            collective_id=0, has_side_effects=True, vmem_limit_bytes=40 * 1024 * 1024
        ),
        name="merge",
    )(*map(hbm, (
        fine_features.reshape(384, COLS), coarse_level, lat_weight.reshape(2, 16, 192),
        vec(lat_gain), vec(lat_shift),
        out_weight.reshape(9, 2, 16, 256), vec(out_gain), vec(out_shift),
        mask_weight.reshape(2, 16, 256), vec(mask_bias),
    )))
    out = pl.pallas_call(
        log_probs_of,
        out_shape=jax.ShapeDtypeStruct((2, 800, 128), f32),
        in_specs=[pl.BlockSpec(memory_space=V)] * 4,
        out_specs=pl.BlockSpec(memory_space=pl.ANY),
        scratch_shapes=[V((2, 800, 128), f32), dma((2,))],
        compiler_params=pltpu.CompilerParams(vmem_limit_bytes=16 * 1024 * 1024),
        name="log_probs",
    )(act, mask_w, bias, queries)
    return out.reshape(2, 200, 1, COLS)


def solution(mesh):
    finer = Mesh(mesh.devices.reshape(8, 2, 2, 4, 2), AXES)
    return jax.shard_map(
        per_device,
        mesh=finer,
        in_specs=(
            P(None, CHAN, BAND, None),
            P(None, CHAN, BAND, None),
            P(CHAN, None),
            P(CHAN),
            P(CHAN),
            P(None, None, CHAN, None),
            P(CHAN),
            P(CHAN),
            P(CHAN, None),
            P(CHAN),
            P(),
        ),
        out_specs=P(None, None, AXES, None),
        check_vma=False,
    )
```

```python
import functools

import jax
import jax.numpy as jnp
from jax import lax
from jax.experimental import pallas as pl
from jax.experimental.pallas import tpu as pltpu
from jax.sharding import Mesh
from jax.sharding import PartitionSpec as P

D = 256
GROUPS = 32
COLS = 512
AXES = ("band_0", "band_1", "band_2", "chan_0", "chan_1")
BAND = AXES[:3]
CHAN = AXES[3:]
MESH = pl.DeviceIdType.MESH
f32, bf16 = jnp.float32, jnp.bfloat16
epsilon = 1e-05

CHAN_OFF = [(dx, dy) for dx in (0, 1, 3, 2) for dy in (1, 0) if (dx, dy) != (0, 0)]
PLANE_OFF = [
    (dx, dh, dl)
    for dx in (2, 1, 3, 0)
    for dh in (1, 0)
    for dl in (1, 0)
    if (dx, dh, dl) != (0, 0, 0)
]
SAME_OFF = [o for o in PLANE_OFF if o[1] == o[2]]
LINE_OFF = [(dz, dc) for dz in (4, 3, 5, 2, 6, 1, 7, 0) for dc in (1, 0) if (dz, dc) != (0, 0)]
DEST = [(1, 0, 1), (0, 1, 0), (1, 1, 1), (0, 0, 0), (1, 0, 0), (0, 1, 1), (1, 1, 0), (0, 0, 1)]
PIECES = (0, 3, 1, 2)


def kernel(
    pixels,
    fine_in, coarse_in, latw_in, lat_gain, lat_shift, outw_in, out_gain, out_shift, maskw_in, mask_bias,
    act_out, mask_out, bias_out,
    fine, coarse, latw, PV, s_in,
    FS, FB, CB, WB, X, C, WL, WC, PB, pstage, LAT, UPS, JS, CO, R,
    plane_src, plane_dst, line_src, line_dst, line_src2, line_dst2,
    s_fine, r_fine, s_coarse, r_coarse, s_latw, r_latw, s_par, r_par, s_w, r_w,
    s_halo, r_halo, s_z, r_z, s_core, r_core, s_plane, r_plane, s_line, r_line, s_row, r_row,
):
    z, yh, core = (lax.axis_index(a) for a in BAND)
    x, yl = (lax.axis_index(a) for a in CHAN)
    me = x * 2 + yl
    fold = lambda v, odd: v + odd * (3 - 2 * v)
    xe = fold(x, yh)
    img = lax.rem(yl + yh, 2)
    pair = (z * 2 + yh) * 8 + xe * 2 + core
    half = lax.rem(z + yh, 2)

    def chan_peer(dx, dy, dc=0):
        return (z, yh, lax.rem(core + dc, 2), lax.rem(x + dx, 4), lax.rem(yl + dy, 2))

    def plane_peer(dx, dh, dl):
        return (z, lax.rem(yh + dh, 2), core, lax.rem(x + dx, 4), lax.rem(yl + dl, 2))

    def line_peer(dz, dc):
        return (lax.rem(z + dz, 8), yh, lax.rem(core + dc, 2), x, yl)

    def pair_owner(g):
        k, p = lax.div(g, 8), lax.rem(g, 8)
        odd = lax.rem(k, 2)
        return (lax.div(k, 2), odd, lax.rem(p, 2), fold(lax.div(p, 2), odd), lax.rem(img + odd, 2))

    above = pair_owner(lax.rem(pair + 127, 128))
    below = pair_owner(lax.rem(pair + 1, 128))
    partner = (z, yh, 1 - core, x, yl)

    def remote(src, dst, send, recv, dev):
        return pltpu.make_async_remote_copy(
            src_ref=src, dst_ref=dst, send_sem=send, recv_sem=recv,
            device_id=dev, device_id_type=MESH,
        )

    barrier = pltpu.get_barrier_semaphore()
    peers = (
        [plane_peer(*o) for o in PLANE_OFF]
        + [line_peer(*o) for o in LINE_OFF]
        + [chan_peer(*o, 1) for o in CHAN_OFF]
        + [above, below]
    )
    for dev in peers:
        pl.semaphore_signal(barrier, inc=1, device_id=dev, device_id_type=MESH)

    loads = [
        pltpu.make_async_copy(src, dst, s_in.at[i])
        for i, (src, dst) in enumerate(
            [(fine_in, fine), (latw_in, latw), (coarse_in, coarse), (outw_in, WB.at[pl.ds(0, 9)]),
             (maskw_in, WB.at[9])]
            + [(v, PV.at[j]) for j, v in enumerate((lat_gain, lat_shift, out_gain, out_shift, mask_bias))]
        )
    ]
    for c in loads:
        c.start()
    loads[0].wait()
    for k in range(4):
        cols = slice(128 * k, 128 * (k + 1))
        FS[384 * k : 384 * (k + 1)] = fine[:, cols].astype(f32)
        for n in range(2):
            for r in range(8):
                FB[n, r, :, cols] = FS[pl.ds(384 * k + 192 * n + r, 24, stride=8), :].astype(bf16)
    loads[1].wait()
    WL[me, core] = latw[core]
    pl.semaphore_wait(barrier, len(peers))

    latw_c, par_c, w_c = [], [], []
    for k, o in enumerate(CHAN_OFF):
        dev = chan_peer(*o)
        latw_c.append(remote(latw.at[core], WL.at[me, core], s_latw.at[k], r_latw.at[k], dev))
        par_c.append(remote(pstage, PB.at[me], s_par.at[k], r_par.at[k], dev))
        w_c.append(remote(WB.at[pl.ds(5 * half, 5), core], WC.at[pl.ds(5 * half, 5), me, core],
                          s_w.at[k], r_w.at[k], dev))
    for c in latw_c:
        c.start()
    shares = []
    for k, (ax, ac, al) in enumerate(DEST):
        xh, dc, dl = lax.rem(x + ax, 2), lax.rem(yl + ac, 2), lax.rem(yl + al, 2)
        xd = fold(2 * core + xh, yh)
        image = lax.rem(dl + yh, 2)
        dev = (z, yh, dc, xd, dl)
        is_self = (xd == x) & (dc == core) & (dl == yl)
        pos = 2 * xh + dc
        cf = remote(FB.at[image, pl.ds(2 * pos, 2)], X.at[pl.ds(1, 2), me], s_fine.at[k], r_fine.at[me], dev)
        cc = remote(CB.at[image, pos], C.at[1, me], s_coarse.at[k], r_coarse.at[me], dev)
        shares.append((is_self, cf, cc, image, pos))

        @pl.when(is_self)
        def _():
            X[pl.ds(1, 2), me] = FB[image, pl.ds(2 * pos, 2)]

        @pl.when(jnp.logical_not(is_self))
        def _():
            cf.start()

    for c in loads[2:]:
        c.wait()
    for n in range(2):
        rows = coarse[n].astype(f32)
        for r in range(4):
            CB[n, r] = rows[:, r, :].astype(bf16)
    pstage[...] = jnp.zeros_like(pstage)
    for j in range(5):
        pstage[j : j + 1, 0:32] = PV[j].astype(f32)
    PB[me] = pstage[...]
    WC[pl.ds(5 * half, 5), me, core] = WB[pl.ds(5 * half, 5), core]
    def wait_shares(buf, width, send, recv):
        for s in range(8):
            @pl.when(jnp.logical_not((s == me) & (lax.div(xe, 2) == core)))
            def _():
                dst = buf.at[pl.ds(1, width), s]
                remote(dst, dst, send.at[s], recv.at[s], partner).wait_recv()

    ci = lax.broadcasted_iota(jnp.int32, (256, COLS), 0)
    cj = lax.broadcasted_iota(jnp.int32, (256, COLS), 1)
    center = lax.shift_right_logical(cj, 1)
    side = jnp.clip(jnp.where(lax.bitwise_and(cj, 1) == 0, center - 1, center + 1), 0, 255)
    widen = (jnp.where(ci == center, 0.75, 0.0) + jnp.where(ci == side, 0.25, 0.0)).astype(bf16)

    def lateral_of(slot):
        rows = X[slot].astype(f32).reshape(192, COLS).astype(bf16)
        return jnp.dot(WL[...].reshape(256, 192), rows, preferred_element_type=f32)

    def row_stats(rows):
        s = q = None
        for row in rows:
            for k in range(COLS // 128):
                t = row[:, 128 * k : 128 * (k + 1)]
                s = t if s is None else s + t
                q = t * t if q is None else q + t * t
        both = jnp.concatenate(
            [jnp.sum(s.reshape(GROUPS, 8, 128), 1), jnp.sum(q.reshape(GROUPS, 8, 128), 1),
             jnp.zeros((64, 128), f32)], 0)
        return jnp.sum(jnp.transpose(both), 0, keepdims=True)

    def scale_shift(total, gain, shift):
        tall = jnp.transpose(jnp.broadcast_to(total, (128, 128)))
        mean = tall[0:32] / pixels
        var = tall[32:64] / pixels - mean * mean
        rstd = lax.rsqrt(var + epsilon)
        spread = lambda v: jnp.broadcast_to(v[:, None, :], (GROUPS, 8, 128)).reshape(D, 128)
        a = spread(rstd) * gain
        return a, shift - spread(mean) * a

    def send_plane(it, offsets):
        done = []
        for k, o in enumerate(PLANE_OFF):
            if o in offsets:
                c = remote(plane_src.at[it], plane_dst.at[it, k], s_plane.at[it, k],
                           r_plane.at[it, k], plane_peer(*o))
                c.start()
                done.append(c)
        return done

    def send_line(it):
        done = []
        for k, o in enumerate(LINE_OFF):
            c = remote(line_src.at[it], line_dst.at[it, k], s_line.at[it, k],
                       r_line.at[it, k], line_peer(*o))
            c.start()
            done.append(c)
        return done

    def line_total(it):
        t = line_src[it]
        for k in range(len(LINE_OFF)):
            t = t + line_dst[it, k]
        return t

    for c in latw_c:
        c.wait_recv()
    latw_core = remote(WL.at[:, core], WL.at[:, core], s_core.at[0], r_core.at[0], partner)
    latw_core.start()
    for is_self, _, cc, image, pos in shares:
        @pl.when(is_self)
        def _():
            C[1, me] = CB[image, pos]

        @pl.when(jnp.logical_not(is_self))
        def _():
            cc.start()


    wait_shares(X, 2, s_fine, r_fine)
    latw_core.wait_recv()
    for c in w_c:
        c.start()
    for c in par_c:
        c.start()
    own_rows = [lateral_of(1), lateral_of(2)]
    LAT[1] = own_rows[0]
    LAT[2] = own_rows[1]
    line_src[0] = row_stats(own_rows)
    line1 = send_line(0)

    halo_c = [
        remote(X.at[1], X.at[3], s_halo.at[0], r_halo.at[0], above),
        remote(X.at[2], X.at[0], s_halo.at[1], r_halo.at[1], below),
    ]
    for c in halo_c:
        c.start()
    wait_shares(C, 1, s_coarse, r_coarse)
    coarse_halo = [
        remote(C.at[1], C.at[2], s_halo.at[2], r_halo.at[2], above),
        remote(C.at[1], C.at[0], s_halo.at[3], r_halo.at[3], below),
    ]
    for c in coarse_halo:
        c.start()

    mine = pl.ds(5 * half, 5)
    yours = pl.ds(5 * (1 - half), 5)
    z_c = []

    def piece_of(part, i):
        return WC.at[part, pl.ds(2 * lax.rem(x + PIECES[i], 4), 2), core]

    def pass_piece(i):
        for k, o in enumerate(CHAN_OFF):
            if (o[0] + PIECES[i]) % 4 == 0:
                w_c[k].wait_recv()
        dev = (line_peer(1, 0), line_peer(7, 0), plane_peer(0, 1, 1), line_peer(1 + 6 * yh, 0))[i]
        c = remote(piece_of(mine, i), piece_of(mine, i), s_z.at[i], r_z.at[i], dev)
        c.start()
        z_c.append(c)

    core_c = []

    def take_piece(i):
        piece = piece_of(yours, i)
        remote(piece, piece, s_z.at[i], r_z.at[i], partner).wait_recv()
        c = remote(piece, piece, s_core.at[2 + i], r_core.at[2 + i], partner)
        c.start()
        core_c.append(c)

    pass_piece(0)
    for c in line1:
        c.wait_recv()
    plane_src[0] = line_total(0)
    plane1 = send_plane(0, SAME_OFF)

    pass_piece(1)
    pass_piece(2)
    pass_piece(3)
    core_mine = remote(WC.at[mine, :, core], WC.at[mine, :, core], s_core.at[1], r_core.at[1], partner)
    core_mine.start()

    widened = lambda r: jnp.dot(C[r].reshape(256, 256), widen, preferred_element_type=f32)
    own_wide = widened(1)
    for c in par_c:
        c.wait_recv()
    turned = jnp.transpose(jnp.concatenate([PB[...].reshape(64, 128), jnp.zeros((64, 128), f32)], 0))

    def param(j):
        col = jnp.concatenate([turned[0:32, 8 * s + j : 8 * s + j + 1] for s in range(8)], 0)
        return jnp.broadcast_to(col, (D, 128))

    for c in halo_c:
        c.wait_recv()
    LAT[0] = lateral_of(0)
    LAT[3] = lateral_of(3)
    take_piece(0)
    take_piece(1)
    for c in coarse_halo:
        c.wait_recv()
    wide = [widened(0), own_wide, widened(2)]
    top = jnp.where(pair == 0, wide[1], wide[0])
    bottom = jnp.where(pair == 127, wide[1], wide[2])
    UPS[0] = 0.75 * top + 0.25 * wide[1]
    UPS[1] = 0.25 * top + 0.75 * wide[1]
    UPS[2] = 0.75 * wide[1] + 0.25 * bottom
    UPS[3] = 0.25 * wide[1] + 0.75 * bottom

    take_piece(2)
    take_piece(3)
    for c in plane1:
        c.wait_recv()
    t = plane_src[0]
    for k, o in enumerate(PLANE_OFF):
        if o in SAME_OFF:
            t = t + plane_dst[0, k]
    a, b = scale_shift(t, param(0), param(1))
    a4 = jnp.concatenate([a] * 4, 1)
    b4 = jnp.concatenate([b] * 4, 1)
    lane = lax.broadcasted_iota(jnp.int32, (D, COLS), 1)
    zero = jnp.zeros((), bf16)
    for s in range(4):
        j = LAT[s] * a4 + b4 + UPS[s]
        if s == 0:
            j = jnp.where(pair == 0, 0.0, j)
        if s == 3:
            j = jnp.where(pair == 127, 0.0, j)
        cols = slice(COLS * s, COLS * (s + 1))
        j = j.astype(bf16)
        JS[0:256, cols] = jnp.where(lane == 0, zero, pltpu.roll(j, 1, 1))
        JS[256:512, cols] = j
        JS[512:768, cols] = jnp.where(lane == COLS - 1, zero, pltpu.roll(j, COLS - 1, 1))

    whole = WC.at[mine, :, 1 - core]
    remote(whole, whole, s_core.at[1], r_core.at[1], partner).wait_recv()
    for i in range(4):
        piece = WC.at[yours, pl.ds(2 * lax.rem(x + PIECES[i], 4), 2), 1 - core]
        remote(piece, piece, s_core.at[2 + i], r_core.at[2 + i], partner).wait_recv()
    xf = lax.rem(2 * xe + core, 4)
    kept = (xf == x) & (lax.div(xe, 2) == core)
    taps = [jnp.concatenate([WC[3 * tap + i].reshape(256, 256) for i in range(3)], 1) for tap in range(3)]
    conv_rows, row_c = [], []
    for step in range(2):
        j = 1 - yl if step == 0 else yl
        acc = None
        for tap in range(3):
            cols = pl.ds(pl.multiple_of(COLS * (tap + j), COLS), COLS)
            term = jnp.dot(taps[tap], JS[:, cols], preferred_element_type=f32)
            acc = term if acc is None else acc + term
        conv_rows.append(acc)
        CO[j] = acc.astype(bf16)
        row_c.append(remote(CO.at[j], R.at[img], s_row.at[step], r_row.at[img],
                            (z, yh, lax.div(xe, 2), xf, j)))
    plane_src[1] = row_stats(conv_rows)
    plane2 = send_plane(1, PLANE_OFF)
    row_c[0].start()

    @pl.when(kept)
    def _():
        R[img] = CO[yl]

    @pl.when(jnp.logical_not(kept))
    def _():
        row_c[1].start()

    gain2, shift2, bias = param(2), param(3), param(4)
    bias_out[...] = bias
    mask_out[...] = WC[9].reshape(256, 256)
    for c in plane2:
        c.wait_recv()
    mine_sum, other_sum = plane_src[1], None
    for k, o in enumerate(PLANE_OFF):
        v = plane_dst[1, k]
        if o in SAME_OFF:
            mine_sum = mine_sum + v
        else:
            other_sum = v if other_sum is None else other_sum + v
    line_src2[...] = jnp.concatenate([mine_sum, other_sum], 0)
    line2 = []
    for k, o in enumerate(LINE_OFF):
        c = remote(line_src2, line_dst2.at[k], s_line.at[1, k], r_line.at[1, k], line_peer(*o))
        c.start()
        line2.append(c)
    for group in (latw_c, par_c, w_c, [latw_core], halo_c, coarse_halo, z_c, core_c, [core_mine], plane1, line1, plane2):
        for c in group:
            c.wait_send()
    for is_self, *cs, _, _ in shares:
        @pl.when(jnp.logical_not(is_self))
        def _():
            for c in cs:
                c.wait_send()

    row_c[0].wait_send()

    @pl.when(jnp.logical_not(kept))
    def _():
        row_c[1].wait_send()

    for n in range(2):
        @pl.when(jnp.logical_not(kept & (img == n)))
        def _():
            remote(R.at[n], R.at[n], s_row.at[n], r_row.at[n], partner).wait_recv()

    for c in line2:
        c.wait_recv()
    both = line_src2[...]
    for k in range(len(LINE_OFF)):
        both = both + line_dst2[k]
    for image, total in ((img, both[0:1]), (1 - img, both[1:2])):
        a, b = scale_shift(total, gain2, shift2)
        act_out[image] = jnp.maximum(
            R[image].astype(f32) * jnp.concatenate([a] * 4, 1) + jnp.concatenate([b] * 4, 1), 0.0
        ).astype(bf16)
    for c in line2:
        c.wait_send()


def log_probs_of(act, mask_w, bias, queries, out, buf, sem):
    bias4 = jnp.concatenate([bias[...]] * 4, 1)
    copies = []
    for n in range(2):
        feat = (jnp.dot(mask_w[...], act[n], preferred_element_type=f32) + bias4).astype(bf16)
        logits = jnp.dot(queries[...], feat, preferred_element_type=f32)
        shifted = logits - jnp.max(logits, 0, keepdims=True)
        res = shifted - jnp.log(jnp.sum(jnp.exp(shifted), 0, keepdims=True))
        for k in range(4):
            buf[n, pl.ds(k, 200, stride=4), :] = res[:, 128 * k : 128 * (k + 1)]
        copies.append(pltpu.make_async_copy(buf.at[n], out.at[n], sem.at[n]))
        copies[n].start()
    for c in copies:
        c.wait()


def per_device(
    fine_features, coarse_level, lat_weight, lat_gain, lat_shift, out_weight, out_gain, out_shift,
    mask_weight, mask_bias, queries,
):
    pixels = float(D // GROUPS * 256 * COLS)
    vec = lambda v: v.reshape(1, 32)
    V = pltpu.VMEM
    dma = pltpu.SemaphoreType.DMA
    hbm = lambda v: pltpu.with_memory_space_constraint(v, pltpu.HBM)
    act, mask_w, bias = pl.pallas_call(
        functools.partial(kernel, pixels),
        out_shape=(
            jax.ShapeDtypeStruct((2, D, COLS), bf16),
            jax.ShapeDtypeStruct((D, D), bf16),
            jax.ShapeDtypeStruct((D, 128), f32),
        ),
        in_specs=[pl.BlockSpec(memory_space=pltpu.HBM)] * 10,
        out_specs=(pl.BlockSpec(memory_space=V),) * 3,
        scratch_shapes=[
            V((384, COLS), bf16),
            V((2, 32, 4, 256), bf16),
            V((2, 16, 192), bf16),
            V((5, 1, 32), bf16),
            dma((10,)),
            V((4 * 384, 128), f32),
            V((2, 8, 24, COLS), bf16),
            V((2, 4, 32, 256), bf16),
            V((10, 2, 16, 256), bf16),
            V((4, 8, 24, COLS), bf16),
            V((3, 8, 32, 256), bf16),
            V((8, 2, 16, 192), bf16),
            V((10, 8, 2, 16, 256), bf16),
            V((8, 8, 128), f32),
            V((8, 128), f32),
            V((4, D, COLS), f32),
            V((4, D, COLS), f32),
            V((3 * D, 4 * COLS), bf16),
            V((2, D, COLS), bf16),
            V((2, D, COLS), bf16),
            V((2, 1, 128), f32),
            V((2, 15, 1, 128), f32),
            V((1, 1, 128), f32),
            V((1, 15, 1, 128), f32),
            V((2, 128), f32),
            V((15, 2, 128), f32),
        ]
        + [dma((8,))] * 4
        + [dma((7,))] * 6
        + [dma((4,))] * 2
        + [dma((4,))] * 2
        + [dma((6,))] * 2
        + [dma((2, 15))] * 4
        + [dma((2,))] * 2,
        compiler_params=pltpu.CompilerParams(
            collective_id=0, has_side_effects=True, vmem_limit_bytes=40 * 1024 * 1024
        ),
        name="merge",
    )(*map(hbm, (
        fine_features.reshape(384, COLS), coarse_level, lat_weight.reshape(2, 16, 192),
        vec(lat_gain), vec(lat_shift),
        out_weight.reshape(9, 2, 16, 256), vec(out_gain), vec(out_shift),
        mask_weight.reshape(2, 16, 256), vec(mask_bias),
    )))
    out = pl.pallas_call(
        log_probs_of,
        out_shape=jax.ShapeDtypeStruct((2, 800, 128), f32),
        in_specs=[pl.BlockSpec(memory_space=V)] * 4,
        out_specs=pl.BlockSpec(memory_space=pl.ANY),
        scratch_shapes=[V((2, 800, 128), f32), dma((2,))],
        compiler_params=pltpu.CompilerParams(vmem_limit_bytes=16 * 1024 * 1024),
        name="log_probs",
    )(act, mask_w, bias, queries)
    return out.reshape(2, 200, 1, COLS)


def solution(mesh):
    finer = Mesh(mesh.devices.reshape(8, 2, 2, 4, 2), AXES)
    return jax.shard_map(
        per_device,
        mesh=finer,
        in_specs=(
            P(None, CHAN, BAND, None),
            P(None, CHAN, BAND, None),
            P(CHAN, None),
            P(CHAN),
            P(CHAN),
            P(None, None, CHAN, None),
            P(CHAN),
            P(CHAN),
            P(CHAN, None),
            P(CHAN),
            P(),
        ),
        out_specs=P(None, None, AXES, None),
        check_vma=False,
    )
```

```python
import functools

import jax
import jax.numpy as jnp
from jax import lax
from jax.experimental import pallas as pl
from jax.experimental.pallas import tpu as pltpu
from jax.sharding import Mesh
from jax.sharding import PartitionSpec as P

D = 256
GROUPS = 32
COLS = 512
AXES = ("band_0", "band_1", "band_2", "chan_0", "chan_1")
BAND = AXES[:3]
CHAN = AXES[3:]
MESH = pl.DeviceIdType.MESH
f32, bf16 = jnp.float32, jnp.bfloat16
epsilon = 1e-05

CHAN_OFF = [(dx, dy) for dx in (0, 1, 3, 2) for dy in (1, 0) if (dx, dy) != (0, 0)]
PLANE_OFF = [
    (dx, dh, dl)
    for dx in (2, 1, 3, 0)
    for dh in (1, 0)
    for dl in (1, 0)
    if (dx, dh, dl) != (0, 0, 0)
]
SAME_OFF = [o for o in PLANE_OFF if o[1] == o[2]]
LINE_OFF = [(dz, dc) for dz in (4, 3, 5, 2, 6, 1, 7, 0) for dc in (1, 0) if (dz, dc) != (0, 0)]
DEST = [(1, 0, 1), (0, 1, 0), (1, 1, 1), (0, 0, 0), (1, 0, 0), (0, 1, 1), (1, 1, 0), (0, 0, 1)]
PARTS = (pl.ds(0, 128), pl.ds(128, 128))
PIECES = (0, 3, 1, 2)


def kernel(
    pixels,
    fine_in, coarse_in, latw_in, lat_gain, lat_shift, outw_in, out_gain, out_shift, maskw_in, mask_bias,
    act_out, mask_out, bias_out,
    fine, coarse, latw, PV, s_in,
    FS, FB, CB, WB, X, C, WL, WC, PB, pstage, LAT, UPS, JS, CO, R,
    plane_src, plane_dst, line_src, line_dst, line_src2, line_dst2,
    s_fine, r_fine, s_coarse, r_coarse, s_latw, r_latw, s_par, r_par, s_w, r_w,
    s_halo, r_halo, s_z, r_z, s_core, r_core, s_plane, r_plane, s_line, r_line, s_row, r_row,
):
    z, yh, core = (lax.axis_index(a) for a in BAND)
    x, yl = (lax.axis_index(a) for a in CHAN)
    me = x * 2 + yl
    fold = lambda v, odd: v + odd * (3 - 2 * v)
    xe = fold(x, yh)
    img = lax.rem(yl + yh, 2)
    pair = (z * 2 + yh) * 8 + xe * 2 + core
    half = lax.rem(z + yh, 2)

    def chan_peer(dx, dy, dc=0):
        return (z, yh, lax.rem(core + dc, 2), lax.rem(x + dx, 4), lax.rem(yl + dy, 2))

    def plane_peer(dx, dh, dl):
        return (z, lax.rem(yh + dh, 2), core, lax.rem(x + dx, 4), lax.rem(yl + dl, 2))

    def line_peer(dz, dc):
        return (lax.rem(z + dz, 8), yh, lax.rem(core + dc, 2), x, yl)

    def pair_owner(g):
        k, p = lax.div(g, 8), lax.rem(g, 8)
        odd = lax.rem(k, 2)
        return (lax.div(k, 2), odd, lax.rem(p, 2), fold(lax.div(p, 2), odd), lax.rem(img + odd, 2))

    above = pair_owner(lax.rem(pair + 127, 128))
    below = pair_owner(lax.rem(pair + 1, 128))
    partner = (z, yh, 1 - core, x, yl)

    def remote(src, dst, send, recv, dev):
        return pltpu.make_async_remote_copy(
            src_ref=src, dst_ref=dst, send_sem=send, recv_sem=recv,
            device_id=dev, device_id_type=MESH,
        )

    barrier = pltpu.get_barrier_semaphore()
    peers = (
        [plane_peer(*o) for o in PLANE_OFF]
        + [line_peer(*o) for o in LINE_OFF]
        + [chan_peer(*o, 1) for o in CHAN_OFF]
        + [above, below]
    )
    for dev in peers:
        pl.semaphore_signal(barrier, inc=1, device_id=dev, device_id_type=MESH)

    loads = [
        pltpu.make_async_copy(src, dst, s_in.at[i])
        for i, (src, dst) in enumerate(
            [(fine_in, fine), (latw_in, latw), (coarse_in, coarse), (outw_in, WB.at[pl.ds(0, 9)]),
             (maskw_in, WB.at[9])]
            + [(v, PV.at[j]) for j, v in enumerate((lat_gain, lat_shift, out_gain, out_shift, mask_bias))]
        )
    ]
    for c in loads:
        c.start()
    loads[0].wait()
    for k in range(4):
        cols = slice(128 * k, 128 * (k + 1))
        FS[384 * k : 384 * (k + 1)] = fine[:, cols].astype(f32)
        for n in range(2):
            for r in range(8):
                FB[n, r, :, cols] = FS[pl.ds(384 * k + 192 * n + r, 24, stride=8), :].astype(bf16)
    loads[1].wait()
    WL[me, core] = latw[core]
    pl.semaphore_wait(barrier, len(peers))

    latw_c, par_c, w_c = [], [], []
    for k, o in enumerate(CHAN_OFF):
        dev = chan_peer(*o)
        latw_c.append(remote(latw.at[core], WL.at[me, core], s_latw.at[k], r_latw.at[k], dev))
        par_c.append(remote(pstage, PB.at[me], s_par.at[k], r_par.at[k], dev))
        w_c.append(remote(WB.at[pl.ds(5 * half, 5), core], WC.at[pl.ds(5 * half, 5), me, core],
                          s_w.at[k], r_w.at[k], dev))
    for c in latw_c:
        c.start()
    shares = []
    for k, (ax, ac, al) in enumerate(DEST):
        xh, dc, dl = lax.rem(x + ax, 2), lax.rem(yl + ac, 2), lax.rem(yl + al, 2)
        xd = fold(2 * core + xh, yh)
        image = lax.rem(dl + yh, 2)
        dev = (z, yh, dc, xd, dl)
        is_self = (xd == x) & (dc == core) & (dl == yl)
        pos = 2 * xh + dc
        cf = remote(FB.at[image, pl.ds(2 * pos, 2)], X.at[pl.ds(1, 2), me], s_fine.at[k], r_fine.at[me], dev)
        cc = remote(CB.at[image, pos], C.at[1, me], s_coarse.at[k], r_coarse.at[me], dev)
        shares.append((is_self, cf, cc, image, pos))

        @pl.when(is_self)
        def _():
            X[pl.ds(1, 2), me] = FB[image, pl.ds(2 * pos, 2)]

        @pl.when(jnp.logical_not(is_self))
        def _():
            cf.start()

    for c in loads[2:]:
        c.wait()
    for n in range(2):
        rows = coarse[n].astype(f32)
        for r in range(4):
            CB[n, r] = rows[:, r, :].astype(bf16)
    pstage[...] = jnp.zeros_like(pstage)
    for j in range(5):
        pstage[j : j + 1, 0:32] = PV[j].astype(f32)
    PB[me] = pstage[...]
    WC[pl.ds(5 * half, 5), me, core] = WB[pl.ds(5 * half, 5), core]
    def wait_shares(buf, width, send, recv):
        for s in range(8):
            @pl.when(jnp.logical_not((s == me) & (lax.div(xe, 2) == core)))
            def _():
                dst = buf.at[pl.ds(1, width), s]
                remote(dst, dst, send.at[s], recv.at[s], partner).wait_recv()

    ci = lax.broadcasted_iota(jnp.int32, (256, COLS), 0)
    cj = lax.broadcasted_iota(jnp.int32, (256, COLS), 1)
    center = lax.shift_right_logical(cj, 1)
    side = jnp.clip(jnp.where(lax.bitwise_and(cj, 1) == 0, center - 1, center + 1), 0, 255)
    widen = (jnp.where(ci == center, 0.75, 0.0) + jnp.where(ci == side, 0.25, 0.0)).astype(bf16)

    def lateral_of(slot):
        rows = X[slot].astype(f32).reshape(192, COLS).astype(bf16)
        return jnp.dot(WL[...].reshape(256, 192), rows, preferred_element_type=f32)

    def row_stats(rows):
        s = q = None
        for row in rows:
            for k in range(COLS // 128):
                t = row[:, 128 * k : 128 * (k + 1)]
                s = t if s is None else s + t
                q = t * t if q is None else q + t * t
        both = jnp.concatenate(
            [jnp.sum(s.reshape(GROUPS, 8, 128), 1), jnp.sum(q.reshape(GROUPS, 8, 128), 1),
             jnp.zeros((64, 128), f32)], 0)
        return jnp.sum(jnp.transpose(both), 0, keepdims=True)

    def scale_shift(total, gain, shift):
        tall = jnp.transpose(jnp.broadcast_to(total, (128, 128)))
        mean = tall[0:32] / pixels
        var = tall[32:64] / pixels - mean * mean
        rstd = lax.rsqrt(var + epsilon)
        spread = lambda v: jnp.broadcast_to(v[:, None, :], (GROUPS, 8, 128)).reshape(D, 128)
        a = spread(rstd) * gain
        return a, shift - spread(mean) * a

    def send_plane(it, offsets):
        done = []
        for k, o in enumerate(PLANE_OFF):
            if o in offsets:
                c = remote(plane_src.at[it], plane_dst.at[it, k], s_plane.at[it, k],
                           r_plane.at[it, k], plane_peer(*o))
                c.start()
                done.append(c)
        return done

    def send_line(it):
        done = []
        for k, o in enumerate(LINE_OFF):
            c = remote(line_src.at[it], line_dst.at[it, k], s_line.at[it, k],
                       r_line.at[it, k], line_peer(*o))
            c.start()
            done.append(c)
        return done

    def line_total(it):
        t = line_src[it]
        for k in range(len(LINE_OFF)):
            t = t + line_dst[it, k]
        return t

    for c in latw_c:
        c.wait_recv()
    latw_core = remote(WL.at[:, core], WL.at[:, core], s_core.at[0], r_core.at[0], partner)
    latw_core.start()
    for is_self, _, cc, image, pos in shares:
        @pl.when(is_self)
        def _():
            C[1, me] = CB[image, pos]

        @pl.when(jnp.logical_not(is_self))
        def _():
            cc.start()


    wait_shares(X, 2, s_fine, r_fine)
    latw_core.wait_recv()
    for c in w_c:
        c.start()
    for c in par_c:
        c.start()
    own_rows = [lateral_of(1), lateral_of(2)]
    LAT[1] = own_rows[0]
    LAT[2] = own_rows[1]
    line_src[0] = row_stats(own_rows)
    line1 = send_line(0)

    halo_c = [
        remote(X.at[1], X.at[3], s_halo.at[0], r_halo.at[0], above),
        remote(X.at[2], X.at[0], s_halo.at[1], r_halo.at[1], below),
    ]
    for c in halo_c:
        c.start()
    wait_shares(C, 1, s_coarse, r_coarse)
    coarse_halo = [
        remote(C.at[1], C.at[2], s_halo.at[2], r_halo.at[2], above),
        remote(C.at[1], C.at[0], s_halo.at[3], r_halo.at[3], below),
    ]
    for c in coarse_halo:
        c.start()

    mine = pl.ds(5 * half, 5)
    yours = pl.ds(5 * (1 - half), 5)
    z_c = []

    def piece_of(part, i):
        return WC.at[part, pl.ds(2 * lax.rem(x + PIECES[i], 4), 2), core]

    def pass_piece(i):
        for k, o in enumerate(CHAN_OFF):
            if (o[0] + PIECES[i]) % 4 == 0:
                w_c[k].wait_recv()
        dev = (line_peer(1, 0), line_peer(7, 0), plane_peer(0, 1, 1), line_peer(1 + 6 * yh, 0))[i]
        c = remote(piece_of(mine, i), piece_of(mine, i), s_z.at[i], r_z.at[i], dev)
        c.start()
        z_c.append(c)

    core_c = []

    def take_piece(i):
        piece = piece_of(yours, i)
        remote(piece, piece, s_z.at[i], r_z.at[i], partner).wait_recv()
        c = remote(piece, piece, s_core.at[2 + i], r_core.at[2 + i], partner)
        c.start()
        core_c.append(c)

    pass_piece(0)
    for c in line1:
        c.wait_recv()
    plane_src[0] = line_total(0)
    plane1 = send_plane(0, SAME_OFF)

    pass_piece(1)
    pass_piece(2)
    pass_piece(3)
    core_mine = remote(WC.at[mine, :, core], WC.at[mine, :, core], s_core.at[1], r_core.at[1], partner)
    core_mine.start()

    widened = lambda r: jnp.dot(C[r].reshape(256, 256), widen, preferred_element_type=f32)
    own_wide = widened(1)
    for c in par_c:
        c.wait_recv()
    turned = jnp.transpose(jnp.concatenate([PB[...].reshape(64, 128), jnp.zeros((64, 128), f32)], 0))

    def param(j):
        col = jnp.concatenate([turned[0:32, 8 * s + j : 8 * s + j + 1] for s in range(8)], 0)
        return jnp.broadcast_to(col, (D, 128))

    for c in halo_c:
        c.wait_recv()
    LAT[0] = lateral_of(0)
    LAT[3] = lateral_of(3)
    take_piece(0)
    take_piece(1)
    for c in coarse_halo:
        c.wait_recv()
    wide = [widened(0), own_wide, widened(2)]
    top = jnp.where(pair == 0, wide[1], wide[0])
    bottom = jnp.where(pair == 127, wide[1], wide[2])
    UPS[0] = 0.75 * top + 0.25 * wide[1]
    UPS[1] = 0.25 * top + 0.75 * wide[1]
    UPS[2] = 0.75 * wide[1] + 0.25 * bottom
    UPS[3] = 0.25 * wide[1] + 0.75 * bottom

    take_piece(2)
    take_piece(3)
    for c in plane1:
        c.wait_recv()
    t = plane_src[0]
    for k, o in enumerate(PLANE_OFF):
        if o in SAME_OFF:
            t = t + plane_dst[0, k]
    a, b = scale_shift(t, param(0), param(1))
    a4 = jnp.concatenate([a] * 4, 1)
    b4 = jnp.concatenate([b] * 4, 1)
    lane = lax.broadcasted_iota(jnp.int32, (D, COLS), 1)
    zero = jnp.zeros((), bf16)
    for s in range(4):
        j = LAT[s] * a4 + b4 + UPS[s]
        if s == 0:
            j = jnp.where(pair == 0, 0.0, j)
        if s == 3:
            j = jnp.where(pair == 127, 0.0, j)
        cols = slice(COLS * s, COLS * (s + 1))
        j = j.astype(bf16)
        JS[0:256, cols] = jnp.where(lane == 0, zero, pltpu.roll(j, 1, 1))
        JS[256:512, cols] = j
        JS[512:768, cols] = jnp.where(lane == COLS - 1, zero, pltpu.roll(j, COLS - 1, 1))

    whole = WC.at[mine, :, 1 - core]
    remote(whole, whole, s_core.at[1], r_core.at[1], partner).wait_recv()
    for i in range(4):
        piece = WC.at[yours, pl.ds(2 * lax.rem(x + PIECES[i], 4), 2), 1 - core]
        remote(piece, piece, s_core.at[2 + i], r_core.at[2 + i], partner).wait_recv()
    xf = lax.rem(2 * xe + core, 4)
    kept = (xf == x) & (lax.div(xe, 2) == core)
    taps = [jnp.concatenate([WC[3 * tap + i].reshape(256, 256) for i in range(3)], 1) for tap in range(3)]
    conv_rows, row_c = [], []
    for step in range(2):
        j = 1 - yl if step == 0 else yl
        acc = None
        for tap in range(3):
            cols = pl.ds(pl.multiple_of(COLS * (tap + j), COLS), COLS)
            term = jnp.dot(taps[tap], JS[:, cols], preferred_element_type=f32)
            acc = term if acc is None else acc + term
        conv_rows.append(acc)
        CO[j] = acc.astype(bf16)
        dev = (z, yh, lax.div(xe, 2), xf, j)
        row_c.append([
            remote(CO.at[j, part], R.at[img, part], s_row.at[step, h], r_row.at[img, h], dev)
            for h, part in enumerate(PARTS)
        ])
    plane_src[1] = row_stats(conv_rows)
    plane2 = send_plane(1, PLANE_OFF)
    @pl.when(kept)
    def _():
        R[img] = CO[yl]

    for h in range(len(PARTS)):
        row_c[0][h].start()

        @pl.when(jnp.logical_not(kept))
        def _():
            row_c[1][h].start()

    gain2, shift2, bias = param(2), param(3), param(4)
    bias_out[...] = bias
    mask_out[...] = WC[9].reshape(256, 256)
    for c in plane2:
        c.wait_recv()
    mine_sum, other_sum = plane_src[1], None
    for k, o in enumerate(PLANE_OFF):
        v = plane_dst[1, k]
        if o in SAME_OFF:
            mine_sum = mine_sum + v
        else:
            other_sum = v if other_sum is None else other_sum + v
    line_src2[...] = jnp.concatenate([mine_sum, other_sum], 0)
    line2 = []
    for k, o in enumerate(LINE_OFF):
        c = remote(line_src2, line_dst2.at[k], s_line.at[1, k], r_line.at[1, k], line_peer(*o))
        c.start()
        line2.append(c)
    for group in (latw_c, par_c, w_c, [latw_core], halo_c, coarse_halo, z_c, core_c, [core_mine], plane1, line1, plane2):
        for c in group:
            c.wait_send()
    for is_self, *cs, _, _ in shares:
        @pl.when(jnp.logical_not(is_self))
        def _():
            for c in cs:
                c.wait_send()

    for c in row_c[0]:
        c.wait_send()

    @pl.when(jnp.logical_not(kept))
    def _():
        for c in row_c[1]:
            c.wait_send()

    for n in range(2):
        @pl.when(jnp.logical_not(kept & (img == n)))
        def _():
            for h, part in enumerate(PARTS):
                remote(R.at[n, part], R.at[n, part], s_row.at[n, h], r_row.at[n, h], partner).wait_recv()

    for c in line2:
        c.wait_recv()
    both = line_src2[...]
    for k in range(len(LINE_OFF)):
        both = both + line_dst2[k]
    for image, total in ((img, both[0:1]), (1 - img, both[1:2])):
        a, b = scale_shift(total, gain2, shift2)
        act_out[image] = jnp.maximum(
            R[image].astype(f32) * jnp.concatenate([a] * 4, 1) + jnp.concatenate([b] * 4, 1), 0.0
        ).astype(bf16)
    for c in line2:
        c.wait_send()


def log_probs_of(act, mask_w, bias, queries, out, buf, sem):
    bias4 = jnp.concatenate([bias[...]] * 4, 1)
    copies = []
    for n in range(2):
        feat = (jnp.dot(mask_w[...], act[n], preferred_element_type=f32) + bias4).astype(bf16)
        logits = jnp.dot(queries[...], feat, preferred_element_type=f32)
        shifted = logits - jnp.max(logits, 0, keepdims=True)
        res = shifted - jnp.log(jnp.sum(jnp.exp(shifted), 0, keepdims=True))
        for k in range(4):
            buf[n, pl.ds(k, 200, stride=4), :] = res[:, 128 * k : 128 * (k + 1)]
        copies.append(pltpu.make_async_copy(buf.at[n], out.at[n], sem.at[n]))
        copies[n].start()
    for c in copies:
        c.wait()


def per_device(
    fine_features, coarse_level, lat_weight, lat_gain, lat_shift, out_weight, out_gain, out_shift,
    mask_weight, mask_bias, queries,
):
    pixels = float(D // GROUPS * 256 * COLS)
    vec = lambda v: v.reshape(1, 32)
    V = pltpu.VMEM
    dma = pltpu.SemaphoreType.DMA
    hbm = lambda v: pltpu.with_memory_space_constraint(v, pltpu.HBM)
    act, mask_w, bias = pl.pallas_call(
        functools.partial(kernel, pixels),
        out_shape=(
            jax.ShapeDtypeStruct((2, D, COLS), bf16),
            jax.ShapeDtypeStruct((D, D), bf16),
            jax.ShapeDtypeStruct((D, 128), f32),
        ),
        in_specs=[pl.BlockSpec(memory_space=pltpu.HBM)] * 10,
        out_specs=(pl.BlockSpec(memory_space=V),) * 3,
        scratch_shapes=[
            V((384, COLS), bf16),
            V((2, 32, 4, 256), bf16),
            V((2, 16, 192), bf16),
            V((5, 1, 32), bf16),
            dma((10,)),
            V((4 * 384, 128), f32),
            V((2, 8, 24, COLS), bf16),
            V((2, 4, 32, 256), bf16),
            V((10, 2, 16, 256), bf16),
            V((4, 8, 24, COLS), bf16),
            V((3, 8, 32, 256), bf16),
            V((8, 2, 16, 192), bf16),
            V((10, 8, 2, 16, 256), bf16),
            V((8, 8, 128), f32),
            V((8, 128), f32),
            V((4, D, COLS), f32),
            V((4, D, COLS), f32),
            V((3 * D, 4 * COLS), bf16),
            V((2, D, COLS), bf16),
            V((2, D, COLS), bf16),
            V((2, 1, 128), f32),
            V((2, 15, 1, 128), f32),
            V((1, 1, 128), f32),
            V((1, 15, 1, 128), f32),
            V((2, 128), f32),
            V((15, 2, 128), f32),
        ]
        + [dma((8,))] * 4
        + [dma((7,))] * 6
        + [dma((4,))] * 2
        + [dma((4,))] * 2
        + [dma((6,))] * 2
        + [dma((2, 15))] * 4
        + [dma((2, 2))] * 2,
        compiler_params=pltpu.CompilerParams(
            collective_id=0, has_side_effects=True, vmem_limit_bytes=40 * 1024 * 1024
        ),
        name="merge",
    )(*map(hbm, (
        fine_features.reshape(384, COLS), coarse_level, lat_weight.reshape(2, 16, 192),
        vec(lat_gain), vec(lat_shift),
        out_weight.reshape(9, 2, 16, 256), vec(out_gain), vec(out_shift),
        mask_weight.reshape(2, 16, 256), vec(mask_bias),
    )))
    out = pl.pallas_call(
        log_probs_of,
        out_shape=jax.ShapeDtypeStruct((2, 800, 128), f32),
        in_specs=[pl.BlockSpec(memory_space=V)] * 4,
        out_specs=pl.BlockSpec(memory_space=pl.ANY),
        scratch_shapes=[V((2, 800, 128), f32), dma((2,))],
        compiler_params=pltpu.CompilerParams(vmem_limit_bytes=16 * 1024 * 1024),
        name="log_probs",
    )(act, mask_w, bias, queries)
    return out.reshape(2, 200, 1, COLS)


def solution(mesh):
    finer = Mesh(mesh.devices.reshape(8, 2, 2, 4, 2), AXES)
    return jax.shard_map(
        per_device,
        mesh=finer,
        in_specs=(
            P(None, CHAN, BAND, None),
            P(None, CHAN, BAND, None),
            P(CHAN, None),
            P(CHAN),
            P(CHAN),
            P(None, None, CHAN, None),
            P(CHAN),
            P(CHAN),
            P(CHAN, None),
            P(CHAN),
            P(),
        ),
        out_specs=P(None, None, AXES, None),
        check_vma=False,
    )
```
